32 devices in a mesh: dp: 8 (over z, y), sp: 4 (over x, core).
Axes of the slice: x: 2, y: 2, z: 4, core: 2. Of those that a mesh axis runs over, the one named last changes fastest.
Arguments:
- tokens: bfloat16 [32, 96, 48, 256], P('dp', 'sp')
- grad_out: bfloat16 [32, 48, 24, 512], P(('dp', 'sp'))
- rel_index: int32 [144, 144], replicated
- norm_merge: bfloat16 [2, 1024], replicated
- w_reduce: bfloat16 [1024, 512], replicated
- norm_attn: bfloat16 [2, 512], replicated
- w_qkv: bfloat16 [512, 1536], replicated
- b_qkv: bfloat16 [1536], replicated
- rel_table: bfloat16 [529, 16], replicated
- w_proj: bfloat16 [512, 512], replicated
- b_proj: bfloat16 [512], replicated
- norm_mlp: bfloat16 [2, 512], replicated
- w_fc1: bfloat16 [512, 2048], replicated
- b_fc1: bfloat16 [2048], replicated
- w_fc2: bfloat16 [2048, 512], replicated
- b_fc2: bfloat16 [512], replicated
Outputs:
- output 1: bfloat16 [32, 48, 24, 512], P(('dp', 'sp'))
- output 2: bfloat16 [32, 96, 48, 256], P('dp', 'sp')
- output 3: float32 [2, 1024], replicated
- output 4: float32 [1024, 512], replicated
- output 5: float32 [2, 512], replicated
- output 6: float32 [512, 1536], replicated
- output 7: float32 [1536], replicated
- output 8: float32 [529, 16], replicated
- output 9: float32 [512, 512], replicated
- output 10: float32 [512], replicated
- output 11: float32 [2, 512], replicated
- output 12: float32 [512, 2048], replicated
- output 13: float32 [2048], replicated
- output 14: float32 [2048, 512], replicated
- output 15: float32 [512], replicated
All inputs are finite; a program needn't handle non-finite values.
Results may differ from the reference program's by a relative error of at most 0.02.
Values are sent between devices in bfloat16 or wider.
A program may use at most 1 GiB of HBM per device.

```python
import functools
import jax
import jax.numpy as jnp
from jax import lax

IMAGES = 32
IMG_ROWS = 96
IMG_COLS = 48
IN_DIM = 256
MODEL_DIM = 512
N_HEADS = 16
HEAD_DIM = 32
FF_DIM = 2048
WINDOW = 12
NORM_EPS = 1e-5
SEQ_LEN = WINDOW * WINDOW
TABLE_LEN = (2 * WINDOW - 1) * (2 * WINDOW - 1)


def normal_draw(draw_key, arr_shape, scale_by):
    return (jax.random.normal(draw_key, arr_shape, jnp.float32) * scale_by).astype(jnp.bfloat16)


def norm_draw(draw_key, width_n):
    norm_noise = jax.random.normal(draw_key, (2, width_n), jnp.float32) * 0.25
    return (norm_noise + jnp.array([[1.0], [0.0]], jnp.float32)).astype(jnp.bfloat16)


def setup_inputs(seed: int = 0) -> dict:
    key_list = jax.random.split(jax.random.key(seed), 16)
    pos_grid = jnp.arange(SEQ_LEN)
    pos_row = pos_grid // WINDOW
    pos_col = pos_grid % WINDOW
    rel_flat = (pos_row[:, None] - pos_row[None, :] + WINDOW - 1) * (2 * WINDOW - 1) + pos_col[:, None] - pos_col[None, :] + WINDOW - 1
    relabel = jax.random.permutation(key_list[2], TABLE_LEN)
    return {
        'tokens': normal_draw(key_list[0], (IMAGES, IMG_ROWS, IMG_COLS, IN_DIM), 1.0),
        'grad_out': normal_draw(key_list[1], (IMAGES, IMG_ROWS // 2, IMG_COLS // 2, MODEL_DIM), 1.0),
        'rel_index': relabel[rel_flat].astype(jnp.int32),
        'norm_merge': norm_draw(key_list[3], 4 * IN_DIM),
        'w_reduce': normal_draw(key_list[4], (4 * IN_DIM, MODEL_DIM), (4 * IN_DIM) ** -0.5),
        'norm_attn': norm_draw(key_list[5], MODEL_DIM),
        'w_qkv': normal_draw(key_list[6], (MODEL_DIM, 3 * MODEL_DIM), MODEL_DIM ** -0.5),
        'b_qkv': normal_draw(key_list[7], (3 * MODEL_DIM,), 0.3),
        'rel_table': normal_draw(key_list[8], (TABLE_LEN, N_HEADS), 1.0),
        'w_proj': normal_draw(key_list[9], (MODEL_DIM, MODEL_DIM), MODEL_DIM ** -0.5),
        'b_proj': normal_draw(key_list[10], (MODEL_DIM,), 1.0),
        'norm_mlp': norm_draw(key_list[11], MODEL_DIM),
        'w_fc1': normal_draw(key_list[12], (MODEL_DIM, FF_DIM), MODEL_DIM ** -0.5),
        'b_fc1': normal_draw(key_list[13], (FF_DIM,), 1.0),
        'w_fc2': normal_draw(key_list[14], (FF_DIM, MODEL_DIM), FF_DIM ** -0.5),
        'b_fc2': normal_draw(key_list[15], (MODEL_DIM,), 1.0),
    }


def store_bf16(values):
    return values.astype(jnp.bfloat16).astype(jnp.float32)


def layer_norm(values, norm_pair):
    row_mean = jnp.mean(values, axis=-1, keepdims=True)
    centred = values - row_mean
    row_var = jnp.mean(centred * centred, axis=-1, keepdims=True)
    return centred * lax.rsqrt(row_var + NORM_EPS) * norm_pair[0] + norm_pair[1]


def band_forward(one_band, weights, rel_index):
    (norm_merge, w_reduce, norm_attn, w_qkv, b_qkv, rel_table, w_proj, b_proj, norm_mlp, w_fc1, b_fc1, w_fc2, b_fc2) = weights
    merged_rows = one_band.shape[0] // 2
    merged_cols = one_band.shape[1] // 2
    win_rows = merged_rows // WINDOW
    win_cols = merged_cols // WINDOW
    merged_in = jnp.concatenate([one_band[0::2, 0::2], one_band[1::2, 0::2], one_band[0::2, 1::2], one_band[1::2, 1::2]], axis=-1)
    merged_in = store_bf16(layer_norm(merged_in, norm_merge))
    h_zero = store_bf16(jnp.einsum('hwk,kd->hwd', merged_in, w_reduce))
    h_zero = h_zero.reshape(win_rows, WINDOW, win_cols, WINDOW, MODEL_DIM).transpose(0, 2, 1, 3, 4).reshape(win_rows * win_cols, SEQ_LEN, MODEL_DIM)
    pos_bias = rel_table[rel_index].transpose(2, 0, 1)
    normed_one = store_bf16(layer_norm(h_zero, norm_attn))
    qkv_all = store_bf16(jnp.einsum('nlc,ck->nlk', normed_one, w_qkv) + b_qkv).reshape(-1, SEQ_LEN, 3, N_HEADS, HEAD_DIM)
    scores = jnp.einsum('nlhe,nmhe->nhlm', qkv_all[:, :, 0], qkv_all[:, :, 1]) * (HEAD_DIM ** -0.5) + pos_bias
    attn_prob = store_bf16(jax.nn.softmax(scores, axis=-1))
    attn_out = store_bf16(jnp.einsum('nhlm,nmhe->nlhe', attn_prob, qkv_all[:, :, 2])).reshape(-1, SEQ_LEN, MODEL_DIM)
    h_one = store_bf16(h_zero + jnp.einsum('nlc,cd->nld', attn_out, w_proj) + b_proj)
    normed_two = store_bf16(layer_norm(h_one, norm_mlp))
    hidden = store_bf16(jax.nn.gelu(jnp.einsum('nlc,cf->nlf', normed_two, w_fc1) + b_fc1, approximate=False))
    out_win = store_bf16(h_one + jnp.einsum('nlf,fd->nld', hidden, w_fc2) + b_fc2)
    return out_win.reshape(win_rows, win_cols, WINDOW, WINDOW, MODEL_DIM).transpose(0, 2, 1, 3, 4).reshape(merged_rows, merged_cols, MODEL_DIM)


def reference(tokens, grad_out, rel_index, norm_merge, w_reduce, norm_attn, w_qkv, b_qkv, rel_table, w_proj, b_proj, norm_mlp, w_fc1, b_fc1, w_fc2, b_fc2):
    weights = tuple(weight.astype(jnp.float32) for weight in (norm_merge, w_reduce, norm_attn, w_qkv, b_qkv, rel_table, w_proj, b_proj, norm_mlp, w_fc1, b_fc1, w_fc2, b_fc2))
    band_fn = functools.partial(band_forward, rel_index=rel_index)
    band_count = IMAGES * (IMG_ROWS // (2 * WINDOW))
    tok_bands = tokens.reshape(band_count, 2 * WINDOW, IMG_COLS, IN_DIM)
    cot_bands = grad_out.reshape(band_count, WINDOW, IMG_COLS // 2, MODEL_DIM)

    def scan_body(grad_acc, band_pair):
        out_band, band_pull = jax.vjp(band_fn, band_pair[0].astype(jnp.float32), weights)
        d_band, d_weights = band_pull(band_pair[1].astype(jnp.float32))
        grad_acc = jax.tree.map(jnp.add, grad_acc, d_weights)
        return grad_acc, (out_band.astype(jnp.bfloat16), d_band.astype(jnp.bfloat16))

    grad_zero = jax.tree.map(jnp.zeros_like, weights)
    weight_grads, per_band = lax.scan(scan_body, grad_zero, (tok_bands, cot_bands))
    result = per_band[0].reshape(IMAGES, IMG_ROWS // 2, IMG_COLS // 2, MODEL_DIM)
    grad_tokens = per_band[1].reshape(IMAGES, IMG_ROWS, IMG_COLS, IN_DIM)
    return (result, grad_tokens, weight_grads[0], weight_grads[1], weight_grads[2], weight_grads[3], weight_grads[4], weight_grads[5], weight_grads[6], weight_grads[7], weight_grads[8], weight_grads[9], weight_grads[10], weight_grads[11], weight_grads[12])
```

```python
import functools
import math
import numpy as np
import jax
import jax.numpy as jnp
from jax import lax
from jax.experimental import pallas as pl
from jax.experimental.pallas import tpu as pltpu
from jax.sharding import PartitionSpec as P

NORM_EPS = 1e-5
BF, F32 = jnp.bfloat16, jnp.float32
VMEM_LIMIT = 60 * 1024 * 1024
HEAD_GROUP = 8
GROUP_ROWS = 4


def dot_nn(a, b):
    return lax.dot_general(a, b, (((1,), (0,)), ((), ())), preferred_element_type=F32)


def dot_nt(a, b):
    return lax.dot_general(a, b, (((1,), (1,)), ((), ())), preferred_element_type=F32)


def dot_tn(a, b):
    return lax.dot_general(a, b, (((0,), (0,)), ((), ())), preferred_element_type=F32)


def norm_hat(x):
    mu = jnp.mean(x, axis=-1, keepdims=True)
    xc = x - mu
    rstd = lax.rsqrt(jnp.mean(xc * xc, axis=-1, keepdims=True) + NORM_EPS)
    return xc * rstd, rstd


def norm_fwd(x, norm_ref):
    hat, rstd = norm_hat(x)
    return hat * norm_ref[0:1, :].astype(F32) + norm_ref[1:2, :].astype(F32), hat, rstd


def norm_bwd(dy, hat, rstd, norm_ref):
    dhat = dy * norm_ref[0:1, :].astype(F32)
    m1 = jnp.mean(dhat, axis=-1, keepdims=True)
    m2 = jnp.mean(dhat * hat, axis=-1, keepdims=True)
    dx = rstd * (dhat - m1 - hat * m2)
    return dx, jnp.sum(dy * hat, axis=0, keepdims=True), jnp.sum(dy, axis=0, keepdims=True)


def head_masks(width, head_dim, dtype):
    lane = lax.broadcasted_iota(jnp.int32, (1, width), 1) // head_dim
    return [jnp.where(lane == h, 1.0, 0.0).astype(dtype) for h in range(width // head_dim)]


def stack_heads(x, masks):
    return jnp.concatenate([x * m for m in masks], axis=0)


def unstack_heads(x, masks, seq):
    total = x[0:seq] * masks[0]
    for h in range(1, len(masks)):
        total = total + x[h * seq:(h + 1) * seq] * masks[h]
    return total


def pos_kernel(table_ref, idx_ref, pos_ref):
    seq = idx_ref.shape[0]
    n_pieces = table_ref.shape[1] // 128
    for g in range(pos_ref.shape[0]):
        wide = jnp.concatenate([idx_ref[...]] * HEAD_GROUP, axis=1)
        for c in range(wide.shape[1] // 128):
            idx = wide[:, c * 128:(c + 1) * 128]
            low, high = idx & 127, idx >> 7
            lane = lax.broadcasted_iota(jnp.int32, idx.shape, 1) + c * 128
            out = jnp.zeros(idx.shape, F32)
            for h in range((c * 128) // seq, (c * 128 + 127) // seq + 1):
                val = jnp.zeros(idx.shape, F32)
                for t in range(n_pieces):
                    row = table_ref[g * HEAD_GROUP + h:g * HEAD_GROUP + h + 1, t * 128:(t + 1) * 128]
                    got = jnp.take_along_axis(jnp.broadcast_to(row, idx.shape), low, axis=1)
                    val = jnp.where(high == t, got, val)
                out = jnp.where((lane >= h * seq) & (lane < (h + 1) * seq), val, out)
            pos_ref[g, :, c * 128:(c + 1) * 128] = out


def fwd_kernel(tok_ref, perm_ref, pos_ref, nm_ref, wr_ref, na_ref, wq_ref, bq_ref, wp_ref, bp_ref,
               raw_ref, h0_ref, qkv_ref, att_ref, lse_ref, h1_ref, *, head_dim, seq):
    dim = h0_ref.shape[2]
    x = tok_ref[0].reshape(-1, tok_ref.shape[3])
    step = perm_ref.shape[0]
    quad = step // 4
    piece = quad // 2
    for g in range(x.shape[0] // step):
        y = dot_nn(perm_ref[...], x[g * step:(g + 1) * step])
        for w in range(2):
            cat = jnp.concatenate([y[p * quad + w * piece:p * quad + (w + 1) * piece] for p in range(4)], axis=1)
            raw_ref[0, w * seq + g * piece:w * seq + (g + 1) * piece, :] = cat.astype(BF)
    merged = norm_fwd(raw_ref[0].astype(F32), nm_ref)[0].astype(BF)
    h0 = dot_nn(merged, wr_ref[...]).astype(BF)
    h0_ref[0] = h0
    a = norm_fwd(h0.astype(F32), na_ref)[0].astype(BF)
    qkv_ref[0] = (dot_nn(a, wq_ref[...]) + bq_ref[...].astype(F32)).astype(BF)
    width = HEAD_GROUP * head_dim
    masks, masks_f = head_masks(width, head_dim, BF), head_masks(width, head_dim, F32)
    scale = head_dim ** -0.5
    for w in range(2):
        rows = slice(w * seq, (w + 1) * seq)
        for g in range(dim // width):
            cols = [slice(t * dim + g * width, t * dim + (g + 1) * width) for t in range(3)]
            q, k, v = (qkv_ref[0, rows, c] for c in cols)
            s = dot_nt(k, stack_heads(q, masks)) * scale + pos_ref[g]
            top = jnp.max(s, axis=0, keepdims=True)
            e = jnp.exp(s - top)
            den = jnp.sum(e, axis=0, keepdims=True)
            prob = (e * (1.0 / den)).astype(BF)
            lse_ref[0, w, g] = top + jnp.log(den)
            att_ref[0, rows, g * width:(g + 1) * width] = unstack_heads(dot_tn(prob, v), masks_f, seq).astype(BF)
    h1 = h0_ref[0].astype(F32) + dot_nn(att_ref[0], wp_ref[...]) + bp_ref[...].astype(F32)
    h1_ref[0] = h1.astype(BF)


def mlp_kernel(h1_ref, cot_ref, perm_ref, nb_ref, w1_ref, b1_ref, w2_ref, b2_ref,
               out_ref, dh1_ref, gw1_ref, gw2_ref, gb1_ref, gb2_ref, gnb_ref,
               hid_s, dpre_s, b_s, cot_s):
    i = pl.program_id(0)
    n = h1_ref.shape[1]

    @pl.when(i == 0)
    def _():
        gb1_ref[...] = jnp.zeros(gb1_ref.shape, F32)
        gb2_ref[...] = jnp.zeros(gb2_ref.shape, F32)
        gnb_ref[...] = jnp.zeros(gnb_ref.shape, F32)

    rows = pl.ds(pl.multiple_of(i * n, n), n)
    h1 = h1_ref[0].astype(F32)
    normed, hat, rstd = norm_fwd(h1, nb_ref)
    nb = normed.astype(BF)
    b_s[rows, :] = nb
    cot = dot_nn(perm_ref[...], cot_ref[0])
    cot_bf = cot.astype(BF)
    cot_s[rows, :] = cot_bf
    gb2_ref[...] += jnp.sum(cot, axis=0, keepdims=True)
    out = h1 + b2_ref[...].astype(F32)
    d_norm = jnp.zeros(h1.shape, F32)
    chunk = 512
    for c in range(w1_ref.shape[1] // chunk):
        cols = slice(c * chunk, (c + 1) * chunk)
        pre = dot_nn(nb, w1_ref[:, cols]) + b1_ref[:, cols].astype(F32)
        phi = 0.5 + 0.5 * lax.erf(pre * math.sqrt(0.5))
        hid = (pre * phi).astype(BF)
        hid_s[rows, cols] = hid
        out = out + dot_nn(hid, w2_ref[cols, :])
        d_act = phi + pre * (jnp.exp(pre * pre * -0.5) * (1.0 / math.sqrt(2.0 * math.pi)))
        d_pre = dot_nt(cot_bf, w2_ref[cols, :]) * d_act
        gb1_ref[:, cols] += jnp.sum(d_pre, axis=0, keepdims=True)
        d_pre_bf = d_pre.astype(BF)
        dpre_s[rows, cols] = d_pre_bf
        d_norm = d_norm + dot_nt(d_pre_bf, w1_ref[:, cols])
    out_ref[0] = dot_tn(perm_ref[...], out.astype(BF)).astype(BF)
    dx, g_gain, g_shift = norm_bwd(d_norm, hat, rstd, nb_ref)
    gnb_ref[0:1, :] += g_gain
    gnb_ref[1:2, :] += g_shift
    dh1_ref[0] = cot + dx

    @pl.when(i == pl.num_programs(0) - 1)
    def _():
        def body(c, carry):
            cols = pl.ds(pl.multiple_of(c * chunk, chunk), chunk)
            gw1_ref[:, cols] = dot_tn(b_s[...], dpre_s[:, cols])
            gw2_ref[cols, :] = dot_tn(hid_s[:, cols], cot_s[...])
            return carry
        lax.fori_loop(0, w1_ref.shape[1] // chunk, body, 0)


def bwd_kernel(dh1_ref, raw_ref, h0_ref, qkv_ref, att_ref, lse_ref, perm_ref, pos_ref, nm_ref, wr_ref, na_ref, wq_ref, wp_ref,
               gtok_ref, gwp_ref, gwq_ref, gwr_ref, gbp_ref, gbq_ref, gna_ref, gnm_ref, gpos_ref,
               att_s, dh1_s, a_s, dqkv_s, m_s, dh0_s, datt_s, dqkv_f, *, head_dim, seq):
    i = pl.program_id(0)
    n = dh1_ref.shape[1]
    dim = h0_ref.shape[2]

    @pl.when(i == 0)
    def _():
        for ref in (gbp_ref, gbq_ref, gna_ref, gnm_ref, gpos_ref):
            ref[...] = jnp.zeros(ref.shape, F32)

    here = pl.ds(pl.multiple_of(i * n, n), n)
    dh1 = dh1_ref[0]
    gbp_ref[...] += jnp.sum(dh1, axis=0, keepdims=True)
    dh1_bf = dh1.astype(BF)
    dh1_s[here, :] = dh1_bf
    att_s[here, :] = att_ref[0]
    datt_s[...] = dot_nt(dh1_bf, wp_ref[...]).astype(BF)
    width = HEAD_GROUP * head_dim
    masks, masks_f = head_masks(width, head_dim, BF), head_masks(width, head_dim, F32)
    scale = head_dim ** -0.5
    for w in range(2):
        rows = slice(w * seq, (w + 1) * seq)
        for g in range(dim // width):
            cols = [slice(t * dim + g * width, t * dim + (g + 1) * width) for t in range(3)]
            q, k, v = (qkv_ref[0, rows, c] for c in cols)
            qm = stack_heads(q, masks)
            dam = stack_heads(datt_s[rows, g * width:(g + 1) * width], masks)
            prob = jnp.exp(dot_nt(k, qm) * scale + pos_ref[g] - lse_ref[0, w, g])
            d_prob = dot_nt(v, dam)
            dqkv_f[rows, cols[2]] = dot_nn(prob.astype(BF), dam)
            delta = jnp.sum(d_prob * prob, axis=0, keepdims=True)
            ds = prob * (d_prob - delta)
            gpos_ref[g] += ds
            ds_bf = (ds * scale).astype(BF)
            dqkv_f[rows, cols[1]] = dot_nn(ds_bf, qm)
            dqkv_f[rows, cols[0]] = unstack_heads(dot_tn(ds_bf, k), masks_f, seq)
    gbq_ref[...] += jnp.sum(dqkv_f[...], axis=0, keepdims=True)
    dqkv_bf = dqkv_f[...].astype(BF)
    dqkv_s[here, :] = dqkv_bf
    d_a = dot_nt(dqkv_bf, wq_ref[...])
    normed, hat, rstd = norm_fwd(h0_ref[0].astype(F32), na_ref)
    a_s[here, :] = normed.astype(BF)
    dx, g_gain, g_shift = norm_bwd(d_a, hat, rstd, na_ref)
    gna_ref[0:1, :] += g_gain
    gna_ref[1:2, :] += g_shift
    dh0_bf = (dh1 + dx).astype(BF)
    dh0_s[here, :] = dh0_bf
    d_m = dot_nt(dh0_bf, wr_ref[...])
    normed, hat, rstd = norm_fwd(raw_ref[0].astype(F32), nm_ref)
    m_s[here, :] = normed.astype(BF)
    dx, g_gain, g_shift = norm_bwd(d_m, hat, rstd, nm_ref)
    gnm_ref[0:1, :] += g_gain
    gnm_ref[1:2, :] += g_shift
    d_raw = dx.astype(BF)
    step = perm_ref.shape[0]
    quad = step // 4
    piece = quad // 2
    chan = d_raw.shape[1] // 4
    tok_rows = step // gtok_ref.shape[2]
    for g in range(seq // piece):
        y = jnp.concatenate([d_raw[w * seq + g * piece:w * seq + (g + 1) * piece, p * chan:(p + 1) * chan]
                             for p in range(4) for w in range(2)], axis=0)
        gtok_ref[0, g * tok_rows:(g + 1) * tok_rows] = dot_tn(perm_ref[...], y).astype(BF).reshape(tok_rows, gtok_ref.shape[2], chan)

    @pl.when(i == pl.num_programs(0) - 1)
    def _():
        gwp_ref[...] = dot_tn(att_s[...], dh1_s[...])

        def body_q(c, carry):
            cols = pl.ds(pl.multiple_of(c * 512, 512), 512)
            gwq_ref[:, cols] = dot_tn(a_s[...], dqkv_s[:, cols])
            return carry
        lax.fori_loop(0, gwq_ref.shape[1] // 512, body_q, 0)

        def body_r(c, carry):
            cols = pl.ds(pl.multiple_of(c * 512, 512), 512)
            gwr_ref[cols, :] = dot_tn(m_s[:, cols], dh0_s[...])
            return carry
        lax.fori_loop(0, gwr_ref.shape[0] // 512, body_r, 0)


def table_kernel(gpos_ref, idx_ref, out_ref, parts_s, *, n_heads):
    m0 = pl.program_id(0)
    count = idx_ref.shape[0]

    @pl.when(m0 == 0)
    def _():
        out_ref[...] = jnp.zeros(out_ref.shape, F32)
    acc = jnp.zeros(out_ref.shape, F32)
    row = lax.broadcasted_iota(jnp.int32, (out_ref.shape[1], idx_ref.shape[1]), 0)
    for j in range(count):
        hot = jnp.where(row == idx_ref[j:j + 1, :], 1.0, 0.0).astype(BF)
        val = gpos_ref[j]
        hi = val.astype(BF)
        rest = val - hi.astype(F32)
        mid = rest.astype(BF)
        low = (rest - mid.astype(F32)).astype(BF)
        acc = acc + dot_nt(jnp.concatenate([hi, mid, low], axis=0), hot)
    out_ref[...] += acc


def whole(shape):
    zeros = (0,) * len(shape)
    return pl.BlockSpec(shape, lambda i: zeros, pipeline_mode=pl.Buffered(1))


def out_whole(shape):
    zeros = (0,) * len(shape)
    return pl.BlockSpec(shape, lambda i: zeros)


def band(shape):
    zeros = (0,) * (len(shape) - 1)
    return pl.BlockSpec((1,) + shape[1:], lambda i: (i,) + zeros)


def sds(shape, dtype):
    return jax.ShapeDtypeStruct(shape, dtype)


def call(kernel, grid, ins, in_specs, outs, out_specs, scratch, flops, name):
    moved = sum(math.prod(a.shape) * a.dtype.itemsize for a in list(ins) + list(outs))
    return pl.pallas_call(
        kernel, grid=grid, in_specs=in_specs, out_specs=out_specs, out_shape=outs, scratch_shapes=scratch, name=name,
        cost_estimate=pl.CostEstimate(flops=flops, bytes_accessed=moved, transcendentals=0),
        compiler_params=pltpu.CompilerParams(vmem_limit_bytes=VMEM_LIMIT, dimension_semantics=("arbitrary",) * len(grid)))(*ins)


def merge_perm(window, cols):
    rows_in = 2 * GROUP_ROWS * cols
    perm = np.zeros((rows_in, rows_in), np.float32)
    out = 0
    for quad in range(4):
        c, r = quad // 2, quad % 2
        for w in range(2):
            for i in range(GROUP_ROWS):
                for j in range(window):
                    perm[out, (2 * i + r) * cols + 2 * (w * window + j) + c] = 1.0
                    out += 1
    return jnp.asarray(perm, BF)


def window_perm(window):
    n = 2 * window * window
    perm = np.zeros((n, n), np.float32)
    for w in range(2):
        for i in range(window):
            for j in range(window):
                perm[(w * window + i) * window + j, (i * 2 + w) * window + j] = 1.0
    return jnp.asarray(perm, BF)


def local_step(tokens, cot, rel_index, weights):
    (norm_merge, w_reduce, norm_attn, w_qkv, b_qkv, rel_table, w_proj, b_proj, norm_mlp, w_fc1, b_fc1, w_fc2, b_fc2) = weights
    nb, tok_rows, tok_cols, chan = tokens.shape
    dim = w_reduce.shape[1]
    ff = w_fc1.shape[1]
    n_heads = rel_table.shape[1]
    head_dim = dim // n_heads
    seq = rel_index.shape[0]
    window = math.isqrt(seq)
    n = 2 * seq
    groups = n_heads // HEAD_GROUP
    lanes = HEAD_GROUP * seq
    table_pad = -(-rel_table.shape[0] // 128) * 128
    perm4, perm_w = merge_perm(window, tok_cols), window_perm(window)
    table_t = jnp.pad(rel_table.astype(F32).T, ((0, 0), (0, table_pad - rel_table.shape[0])))
    idx_t = rel_index.T
    row = lambda x: x.reshape(1, -1)

    pos = call(pos_kernel, (1,), (table_t, idx_t), [whole(table_t.shape), whole(idx_t.shape)],
               [sds((groups, seq, lanes), F32)], [out_whole((groups, seq, lanes))], [], 10**7, "pos")[0]

    ins = (tokens, perm4, pos, norm_merge, w_reduce, norm_attn, w_qkv, row(b_qkv), w_proj, row(b_proj))
    outs = [sds((nb, n, 4 * chan), BF), sds((nb, n, dim), BF), sds((nb, n, 3 * dim), BF), sds((nb, n, dim), BF),
            sds((nb, 2, groups, 1, lanes), F32), sds((nb, n, dim), BF)]
    raw, h0, qkv, att, lse, h1 = call(
        functools.partial(fwd_kernel, head_dim=head_dim, seq=seq), (nb,), ins,
        [band(tokens.shape)] + [whole(a.shape) for a in ins[1:]], outs, [band(o.shape) for o in outs], [], 8 * 10**9, "fwd")

    ins = (h1, cot.reshape(nb, n, dim), perm_w, norm_mlp, w_fc1, row(b_fc1), w_fc2, row(b_fc2))
    outs = [sds((nb, n, dim), BF), sds((nb, n, dim), F32), sds((dim, ff), F32), sds((ff, dim), F32), sds((1, ff), F32), sds((1, dim), F32), sds((2, dim), F32)]
    result, dh1, g_w1, g_w2, g_b1, g_b2, g_nb = call(
        mlp_kernel, (nb,), ins, [band(ins[0].shape), band(ins[1].shape)] + [whole(a.shape) for a in ins[2:]],
        outs, [band(outs[0].shape), band(outs[1].shape)] + [out_whole(o.shape) for o in outs[2:]],
        [pltpu.VMEM((nb * n, ff), BF), pltpu.VMEM((nb * n, ff), BF), pltpu.VMEM((nb * n, dim), BF), pltpu.VMEM((nb * n, dim), BF)],
        16 * 10**9, "mlp")

    ins = (dh1, raw, h0, qkv, att, lse, perm4, pos, norm_merge, w_reduce, norm_attn, w_qkv, w_proj)
    outs = [sds(tokens.shape, BF), sds((dim, dim), F32), sds((dim, 3 * dim), F32), sds((4 * chan, dim), F32), sds((1, dim), F32),
            sds((1, 3 * dim), F32), sds((2, dim), F32), sds((2, 4 * chan), F32), sds((groups, seq, lanes), F32)]
    g_tok, g_wp, g_wq, g_wr, g_bp, g_bq, g_na, g_nm, g_pos = call(
        functools.partial(bwd_kernel, head_dim=head_dim, seq=seq), (nb,), ins,
        [band(a.shape) for a in ins[:6]] + [whole(a.shape) for a in ins[6:]],
        outs, [band(outs[0].shape)] + [out_whole(o.shape) for o in outs[1:]],
        [pltpu.VMEM((nb * n, dim), BF), pltpu.VMEM((nb * n, dim), BF), pltpu.VMEM((nb * n, dim), BF), pltpu.VMEM((nb * n, 3 * dim), BF),
         pltpu.VMEM((nb * n, 4 * chan), BF), pltpu.VMEM((nb * n, dim), BF), pltpu.VMEM((n, dim), BF), pltpu.VMEM((n, 3 * dim), F32)],
        16 * 10**9, "bwd")

    g_pos = g_pos.reshape(groups, seq, HEAD_GROUP, seq).transpose(1, 0, 2, 3).reshape(seq, n_heads, seq)
    block = 8
    parts = call(functools.partial(table_kernel, n_heads=n_heads), (seq // block,), (g_pos, idx_t),
                 [pl.BlockSpec((block, n_heads, seq), lambda i: (i, 0, 0)), pl.BlockSpec((block, seq), lambda i: (i, 0))],
                 [sds((3 * n_heads, table_pad), F32)], [out_whole((3 * n_heads, table_pad))], [pltpu.VMEM((8, 128), F32)], 10**9, "table")[0]
    g_table = parts.reshape(3, n_heads, table_pad).sum(0).T[:rel_table.shape[0]]
    return result, g_tok, (g_nm, g_wr, g_na, g_wq, g_bq[0], g_table, g_wp, g_bp[0], g_nb, g_w1, g_b1[0], g_w2, g_b2[0])


def solution(mesh):
    def device_fn(tokens, grad_out, rel_index, *weights):
        nb = mesh.shape['sp']
        cot = lax.all_to_all(grad_out, 'sp', 1, 0, tiled=True)
        result, g_tok, grads = local_step(tokens, cot, rel_index, weights)
        result = lax.all_to_all(result.reshape(cot.shape), 'sp', 0, 1, tiled=True)
        total = lax.psum(grads, ('dp', 'sp'))
        return (result, g_tok) + tuple(total)

    rep_specs = (P(),) * 13
    return jax.shard_map(device_fn, mesh=mesh, in_specs=(P('dp', 'sp'), P(('dp', 'sp')), P()) + rep_specs, out_specs=(P(('dp', 'sp')), P('dp', 'sp')) + rep_specs, check_vma=False)
```

```python
import functools
import math
import numpy as np
import jax
import jax.numpy as jnp
from jax import lax
from jax.experimental import pallas as pl
from jax.experimental.pallas import tpu as pltpu
from jax.sharding import PartitionSpec as P

NORM_EPS = 1e-5
BF, F32 = jnp.bfloat16, jnp.float32
VMEM_LIMIT = 60 * 1024 * 1024
HEAD_GROUP = 8
GROUP_ROWS = 4


def dot_nn(a, b):
    return lax.dot_general(a, b, (((1,), (0,)), ((), ())), preferred_element_type=F32)


def dot_nt(a, b):
    return lax.dot_general(a, b, (((1,), (1,)), ((), ())), preferred_element_type=F32)


def dot_tn(a, b):
    return lax.dot_general(a, b, (((0,), (0,)), ((), ())), preferred_element_type=F32)


def norm_hat(x):
    mu = jnp.mean(x, axis=-1, keepdims=True)
    xc = x - mu
    rstd = lax.rsqrt(jnp.mean(xc * xc, axis=-1, keepdims=True) + NORM_EPS)
    return xc * rstd, rstd


def norm_fwd(x, norm_ref):
    hat, rstd = norm_hat(x)
    return hat * norm_ref[0:1, :].astype(F32) + norm_ref[1:2, :].astype(F32), hat, rstd


def norm_bwd(dy, hat, rstd, norm_ref):
    dhat = dy * norm_ref[0:1, :].astype(F32)
    m1 = jnp.mean(dhat, axis=-1, keepdims=True)
    m2 = jnp.mean(dhat * hat, axis=-1, keepdims=True)
    dx = rstd * (dhat - m1 - hat * m2)
    return dx, jnp.sum(dy * hat, axis=0, keepdims=True), jnp.sum(dy, axis=0, keepdims=True)


def head_masks(width, head_dim, dtype):
    lane = lax.broadcasted_iota(jnp.int32, (1, width), 1) // head_dim
    return [jnp.where(lane == h, 1.0, 0.0).astype(dtype) for h in range(width // head_dim)]


def stack_heads(x, masks):
    return jnp.concatenate([x * m for m in masks], axis=0)


def unstack_heads(x, masks, seq):
    total = x[0:seq] * masks[0]
    for h in range(1, len(masks)):
        total = total + x[h * seq:(h + 1) * seq] * masks[h]
    return total


def pack(ref, at, value):
    ref[at] = value[:256]
    ref[at + 1] = value[256:]


def pos_kernel(table_ref, idx_ref, pos_ref):
    seq = idx_ref.shape[0]
    n_pieces = table_ref.shape[1] // 128
    for g in range(pos_ref.shape[0]):
        wide = jnp.concatenate([idx_ref[...]] * HEAD_GROUP, axis=1)
        for c in range(wide.shape[1] // 128):
            idx = wide[:, c * 128:(c + 1) * 128]
            low, high = idx & 127, idx >> 7
            lane = lax.broadcasted_iota(jnp.int32, idx.shape, 1) + c * 128
            out = jnp.zeros(idx.shape, F32)
            for h in range((c * 128) // seq, (c * 128 + 127) // seq + 1):
                val = jnp.zeros(idx.shape, F32)
                for t in range(n_pieces):
                    row = table_ref[g * HEAD_GROUP + h:g * HEAD_GROUP + h + 1, t * 128:(t + 1) * 128]
                    got = jnp.take_along_axis(jnp.broadcast_to(row, idx.shape), low, axis=1)
                    val = jnp.where(high == t, got, val)
                out = jnp.where((lane >= h * seq) & (lane < (h + 1) * seq), val, out)
            pos_ref[g, :, c * 128:(c + 1) * 128] = out


def fwd_kernel(tok_ref, perm_ref, pos_ref, nm_ref, wr_ref, na_ref, wq_ref, bq_ref, wp_ref, bp_ref,
               raw_ref, h0_ref, qkv_ref, att_ref, lse_ref, h1_ref, *, head_dim, seq):
    dim = h0_ref.shape[2]
    x = tok_ref[0].reshape(-1, tok_ref.shape[3])
    step = perm_ref.shape[0]
    quad = step // 4
    piece = quad // 2
    for g in range(x.shape[0] // step):
        y = dot_nn(perm_ref[...], x[g * step:(g + 1) * step])
        for w in range(2):
            cat = jnp.concatenate([y[p * quad + w * piece:p * quad + (w + 1) * piece] for p in range(4)], axis=1)
            raw_ref[0, w * seq + g * piece:w * seq + (g + 1) * piece, :] = cat.astype(BF)
    merged = norm_fwd(raw_ref[0].astype(F32), nm_ref)[0].astype(BF)
    h0 = dot_nn(merged, wr_ref[...]).astype(BF)
    h0_ref[0] = h0
    a = norm_fwd(h0.astype(F32), na_ref)[0].astype(BF)
    qkv_ref[0] = (dot_nn(a, wq_ref[...]) + bq_ref[...].astype(F32)).astype(BF)
    width = HEAD_GROUP * head_dim
    masks, masks_f = head_masks(width, head_dim, BF), head_masks(width, head_dim, F32)
    scale = head_dim ** -0.5
    for w in range(2):
        rows = slice(w * seq, (w + 1) * seq)
        for g in range(dim // width):
            cols = [slice(t * dim + g * width, t * dim + (g + 1) * width) for t in range(3)]
            q, k, v = (qkv_ref[0, rows, c] for c in cols)
            s = dot_nt(k, stack_heads(q, masks)) * scale + pos_ref[g]
            top = jnp.max(s, axis=0, keepdims=True)
            e = jnp.exp(s - top)
            den = jnp.sum(e, axis=0, keepdims=True)
            prob = (e * (1.0 / den)).astype(BF)
            lse_ref[0, w, g] = top + jnp.log(den)
            att_ref[0, rows, g * width:(g + 1) * width] = unstack_heads(dot_tn(prob, v), masks_f, seq).astype(BF)
    h1 = h0_ref[0].astype(F32) + dot_nn(att_ref[0], wp_ref[...]) + bp_ref[...].astype(F32)
    h1_ref[0] = h1.astype(BF)


def mlp_kernel(h1_ref, cot_ref, perm_ref, nb_ref, w1_ref, b1_ref, w2_ref, b2_ref,
               out_ref, dh1_ref, gw_ref, gb1_ref, gb2_ref, gnb_ref,
               hid_s, dpre_s, b_s, cot_s):
    i = pl.program_id(0)
    n = h1_ref.shape[1]

    @pl.when(i == 0)
    def _():
        gb1_ref[...] = jnp.zeros(gb1_ref.shape, F32)
        gb2_ref[...] = jnp.zeros(gb2_ref.shape, F32)
        gnb_ref[...] = jnp.zeros(gnb_ref.shape, F32)

    rows = pl.ds(pl.multiple_of(i * n, n), n)
    h1 = h1_ref[0].astype(F32)
    normed, hat, rstd = norm_fwd(h1, nb_ref)
    nb = normed.astype(BF)
    b_s[rows, :] = nb
    cot = dot_nn(perm_ref[...], cot_ref[0])
    cot_bf = cot.astype(BF)
    cot_s[rows, :] = cot_bf
    gb2_ref[...] += jnp.sum(cot, axis=0, keepdims=True)
    out = h1 + b2_ref[...].astype(F32)
    d_norm = jnp.zeros(h1.shape, F32)
    chunk = 512
    for c in range(w1_ref.shape[1] // chunk):
        cols = slice(c * chunk, (c + 1) * chunk)
        pre = dot_nn(nb, w1_ref[:, cols]) + b1_ref[:, cols].astype(F32)
        phi = 0.5 + 0.5 * lax.erf(pre * math.sqrt(0.5))
        hid = (pre * phi).astype(BF)
        hid_s[rows, cols] = hid
        out = out + dot_nn(hid, w2_ref[cols, :])
        d_act = phi + pre * (jnp.exp(pre * pre * -0.5) * (1.0 / math.sqrt(2.0 * math.pi)))
        d_pre = dot_nt(cot_bf, w2_ref[cols, :]) * d_act
        gb1_ref[:, cols] += jnp.sum(d_pre, axis=0, keepdims=True)
        d_pre_bf = d_pre.astype(BF)
        dpre_s[rows, cols] = d_pre_bf
        d_norm = d_norm + dot_nt(d_pre_bf, w1_ref[:, cols])
    out_ref[0] = dot_tn(perm_ref[...], out.astype(BF)).astype(BF)
    dx, g_gain, g_shift = norm_bwd(d_norm, hat, rstd, nb_ref)
    gnb_ref[0:1, :] += g_gain
    gnb_ref[1:2, :] += g_shift
    dh1_ref[0] = cot + dx

    @pl.when(i == pl.num_programs(0) - 1)
    def _():
        def body(c, carry):
            cols = pl.ds(pl.multiple_of(c * chunk, chunk), chunk)
            pack(gw_ref, 2 * c, dot_tn(b_s[...], dpre_s[:, cols]))
            pack(gw_ref, 2 * (w1_ref.shape[1] // chunk + c), dot_tn(hid_s[:, cols], cot_s[...]))
            return carry
        lax.fori_loop(0, w1_ref.shape[1] // chunk, body, 0)


def bwd_kernel(dh1_ref, raw_ref, h0_ref, qkv_ref, att_ref, lse_ref, perm_ref, pos_ref, nm_ref, wr_ref, na_ref, wq_ref, wp_ref,
               gtok_ref, gw_ref, gbp_ref, gbq_ref, gna_ref, gnm_ref, gpos_ref,
               att_s, dh1_s, a_s, dqkv_s, m_s, dh0_s, datt_s, dqkv_f, *, head_dim, seq):
    i = pl.program_id(0)
    n = dh1_ref.shape[1]
    dim = h0_ref.shape[2]

    @pl.when(i == 0)
    def _():
        for ref in (gbp_ref, gbq_ref, gna_ref, gnm_ref, gpos_ref):
            ref[...] = jnp.zeros(ref.shape, F32)

    here = pl.ds(pl.multiple_of(i * n, n), n)
    dh1 = dh1_ref[0]
    gbp_ref[...] += jnp.sum(dh1, axis=0, keepdims=True)
    dh1_bf = dh1.astype(BF)
    dh1_s[here, :] = dh1_bf
    att_s[here, :] = att_ref[0]
    datt_s[...] = dot_nt(dh1_bf, wp_ref[...]).astype(BF)
    width = HEAD_GROUP * head_dim
    masks, masks_f = head_masks(width, head_dim, BF), head_masks(width, head_dim, F32)
    scale = head_dim ** -0.5
    for w in range(2):
        rows = slice(w * seq, (w + 1) * seq)
        for g in range(dim // width):
            cols = [slice(t * dim + g * width, t * dim + (g + 1) * width) for t in range(3)]
            q, k, v = (qkv_ref[0, rows, c] for c in cols)
            qm = stack_heads(q, masks)
            dam = stack_heads(datt_s[rows, g * width:(g + 1) * width], masks)
            prob = jnp.exp(dot_nt(k, qm) * scale + pos_ref[g] - lse_ref[0, w, g])
            d_prob = dot_nt(v, dam)
            dqkv_f[rows, cols[2]] = dot_nn(prob.astype(BF), dam)
            delta = jnp.sum(d_prob * prob, axis=0, keepdims=True)
            ds = prob * (d_prob - delta)
            gpos_ref[g] += ds
            ds_bf = (ds * scale).astype(BF)
            dqkv_f[rows, cols[1]] = dot_nn(ds_bf, qm)
            dqkv_f[rows, cols[0]] = unstack_heads(dot_tn(ds_bf, k), masks_f, seq)
    gbq_ref[...] += jnp.sum(dqkv_f[...], axis=0, keepdims=True)
    dqkv_bf = dqkv_f[...].astype(BF)
    dqkv_s[here, :] = dqkv_bf
    d_a = dot_nt(dqkv_bf, wq_ref[...])
    normed, hat, rstd = norm_fwd(h0_ref[0].astype(F32), na_ref)
    a_s[here, :] = normed.astype(BF)
    dx, g_gain, g_shift = norm_bwd(d_a, hat, rstd, na_ref)
    gna_ref[0:1, :] += g_gain
    gna_ref[1:2, :] += g_shift
    dh0_bf = (dh1 + dx).astype(BF)
    dh0_s[here, :] = dh0_bf
    d_m = dot_nt(dh0_bf, wr_ref[...])
    normed, hat, rstd = norm_fwd(raw_ref[0].astype(F32), nm_ref)
    m_s[here, :] = normed.astype(BF)
    dx, g_gain, g_shift = norm_bwd(d_m, hat, rstd, nm_ref)
    gnm_ref[0:1, :] += g_gain
    gnm_ref[1:2, :] += g_shift
    d_raw = dx.astype(BF)
    step = perm_ref.shape[0]
    quad = step // 4
    piece = quad // 2
    chan = d_raw.shape[1] // 4
    tok_rows = step // gtok_ref.shape[2]
    for g in range(seq // piece):
        y = jnp.concatenate([d_raw[w * seq + g * piece:w * seq + (g + 1) * piece, p * chan:(p + 1) * chan]
                             for p in range(4) for w in range(2)], axis=0)
        gtok_ref[0, g * tok_rows:(g + 1) * tok_rows] = dot_tn(perm_ref[...], y).astype(BF).reshape(tok_rows, gtok_ref.shape[2], chan)

    @pl.when(i == pl.num_programs(0) - 1)
    def _():
        n_red = m_s.shape[1] // 512
        n_qkv = dqkv_s.shape[1] // 512

        def body_r(c, carry):
            cols = pl.ds(pl.multiple_of(c * 512, 512), 512)
            pack(gw_ref, 2 * c, dot_tn(m_s[:, cols], dh0_s[...]))
            return carry
        lax.fori_loop(0, n_red, body_r, 0)

        def body_q(c, carry):
            cols = pl.ds(pl.multiple_of(c * 512, 512), 512)
            pack(gw_ref, 2 * (n_red + c), dot_tn(a_s[...], dqkv_s[:, cols]))
            return carry
        lax.fori_loop(0, n_qkv, body_q, 0)
        pack(gw_ref, 2 * (n_red + n_qkv), dot_tn(att_s[...], dh1_s[...]))


def table_kernel(gpos_ref, idx_ref, out_ref, parts_s, *, n_heads):
    m0 = pl.program_id(0)
    count = idx_ref.shape[0]

    @pl.when(m0 == 0)
    def _():
        out_ref[...] = jnp.zeros(out_ref.shape, F32)
    acc = jnp.zeros(out_ref.shape, F32)
    row = lax.broadcasted_iota(jnp.int32, (out_ref.shape[1], idx_ref.shape[1]), 0)
    for j in range(count):
        hot = jnp.where(row == idx_ref[j:j + 1, :], 1.0, 0.0).astype(BF)
        val = gpos_ref[j]
        hi = val.astype(BF)
        rest = val - hi.astype(F32)
        mid = rest.astype(BF)
        low = (rest - mid.astype(F32)).astype(BF)
        acc = acc + dot_nt(jnp.concatenate([hi, mid, low], axis=0), hot)
    out_ref[...] += acc


def whole(shape):
    zeros = (0,) * len(shape)
    return pl.BlockSpec(shape, lambda i: zeros, pipeline_mode=pl.Buffered(1))


def out_whole(shape):
    zeros = (0,) * len(shape)
    return pl.BlockSpec(shape, lambda i: zeros)


def band(shape):
    zeros = (0,) * (len(shape) - 1)
    return pl.BlockSpec((1,) + shape[1:], lambda i: (i,) + zeros)


def sds(shape, dtype):
    return jax.ShapeDtypeStruct(shape, dtype)


def call(kernel, grid, ins, in_specs, outs, out_specs, scratch, flops, name):
    moved = sum(math.prod(a.shape) * a.dtype.itemsize for a in list(ins) + list(outs))
    return pl.pallas_call(
        kernel, grid=grid, in_specs=in_specs, out_specs=out_specs, out_shape=outs, scratch_shapes=scratch, name=name,
        cost_estimate=pl.CostEstimate(flops=flops, bytes_accessed=moved, transcendentals=0),
        compiler_params=pltpu.CompilerParams(vmem_limit_bytes=VMEM_LIMIT, dimension_semantics=("arbitrary",) * len(grid)))(*ins)


def merge_perm(window, cols):
    rows_in = 2 * GROUP_ROWS * cols
    perm = np.zeros((rows_in, rows_in), np.float32)
    out = 0
    for quad in range(4):
        c, r = quad // 2, quad % 2
        for w in range(2):
            for i in range(GROUP_ROWS):
                for j in range(window):
                    perm[out, (2 * i + r) * cols + 2 * (w * window + j) + c] = 1.0
                    out += 1
    return jnp.asarray(perm, BF)


def window_perm(window):
    n = 2 * window * window
    perm = np.zeros((n, n), np.float32)
    for w in range(2):
        for i in range(window):
            for j in range(window):
                perm[(w * window + i) * window + j, (i * 2 + w) * window + j] = 1.0
    return jnp.asarray(perm, BF)


def local_step(tokens, cot, rel_index, weights):
    (norm_merge, w_reduce, norm_attn, w_qkv, b_qkv, rel_table, w_proj, b_proj, norm_mlp, w_fc1, b_fc1, w_fc2, b_fc2) = weights
    nb, tok_rows, tok_cols, chan = tokens.shape
    dim = w_reduce.shape[1]
    ff = w_fc1.shape[1]
    n_heads = rel_table.shape[1]
    head_dim = dim // n_heads
    seq = rel_index.shape[0]
    window = math.isqrt(seq)
    n = 2 * seq
    groups = n_heads // HEAD_GROUP
    lanes = HEAD_GROUP * seq
    table_pad = -(-rel_table.shape[0] // 128) * 128
    perm4, perm_w = merge_perm(window, tok_cols), window_perm(window)
    table_t = jnp.pad(rel_table.astype(F32).T, ((0, 0), (0, table_pad - rel_table.shape[0])))
    idx_t = rel_index.T
    row = lambda x: x.reshape(1, -1)

    pos = call(pos_kernel, (1,), (table_t, idx_t), [whole(table_t.shape), whole(idx_t.shape)],
               [sds((groups, seq, lanes), F32)], [out_whole((groups, seq, lanes))], [], 10**7, "pos")[0]

    ins = (tokens, perm4, pos, norm_merge, w_reduce, norm_attn, w_qkv, row(b_qkv), w_proj, row(b_proj))
    outs = [sds((nb, n, 4 * chan), BF), sds((nb, n, dim), BF), sds((nb, n, 3 * dim), BF), sds((nb, n, dim), BF),
            sds((nb, 2, groups, 1, lanes), F32), sds((nb, n, dim), BF)]
    raw, h0, qkv, att, lse, h1 = call(
        functools.partial(fwd_kernel, head_dim=head_dim, seq=seq), (nb,), ins,
        [band(tokens.shape)] + [whole(a.shape) for a in ins[1:]], outs, [band(o.shape) for o in outs], [], 8 * 10**9, "fwd")

    ins = (h1, cot.reshape(nb, n, dim), perm_w, norm_mlp, w_fc1, row(b_fc1), w_fc2, row(b_fc2))
    outs = [sds((nb, n, dim), BF), sds((nb, n, dim), F32), sds((4 * ff // 512, 256, 512), F32), sds((1, ff), F32), sds((1, dim), F32), sds((2, dim), F32)]
    result, dh1, gw_mlp, g_b1, g_b2, g_nb = call(
        mlp_kernel, (nb,), ins, [band(ins[0].shape), band(ins[1].shape)] + [whole(a.shape) for a in ins[2:]],
        outs, [band(outs[0].shape), band(outs[1].shape)] + [out_whole(o.shape) for o in outs[2:]],
        [pltpu.VMEM((nb * n, ff), BF), pltpu.VMEM((nb * n, ff), BF), pltpu.VMEM((nb * n, dim), BF), pltpu.VMEM((nb * n, dim), BF)],
        16 * 10**9, "mlp")

    ins = (dh1, raw, h0, qkv, att, lse, perm4, pos, norm_merge, w_reduce, norm_attn, w_qkv, w_proj)
    outs = [sds(tokens.shape, BF), sds((2 * (dim + 3 * dim + 4 * chan) // 512, 256, 512), F32), sds((1, dim), F32),
            sds((1, 3 * dim), F32), sds((2, dim), F32), sds((2, 4 * chan), F32), sds((groups, seq, lanes), F32)]
    g_tok, gw_att, g_bp, g_bq, g_na, g_nm, g_pos = call(
        functools.partial(bwd_kernel, head_dim=head_dim, seq=seq), (nb,), ins,
        [band(a.shape) for a in ins[:6]] + [whole(a.shape) for a in ins[6:]],
        outs, [band(outs[0].shape)] + [out_whole(o.shape) for o in outs[1:]],
        [pltpu.VMEM((nb * n, dim), BF), pltpu.VMEM((nb * n, dim), BF), pltpu.VMEM((nb * n, dim), BF), pltpu.VMEM((nb * n, 3 * dim), BF),
         pltpu.VMEM((nb * n, 4 * chan), BF), pltpu.VMEM((nb * n, dim), BF), pltpu.VMEM((n, dim), BF), pltpu.VMEM((n, 3 * dim), F32)],
        16 * 10**9, "bwd")

    g_pos = g_pos.reshape(groups, seq, HEAD_GROUP, seq).transpose(1, 0, 2, 3).reshape(seq, n_heads, seq)
    block = 8
    parts = call(functools.partial(table_kernel, n_heads=n_heads), (seq // block,), (g_pos, idx_t),
                 [pl.BlockSpec((block, n_heads, seq), lambda i: (i, 0, 0)), pl.BlockSpec((block, seq), lambda i: (i, 0))],
                 [sds((3 * n_heads, table_pad), F32)], [out_whole((3 * n_heads, table_pad))], [pltpu.VMEM((8, 128), F32)], 10**9, "table")[0]
    g_table = parts.reshape(3, n_heads, table_pad).sum(0)
    small = jnp.concatenate([x.reshape(-1) for x in (g_nm, g_na, g_nb, g_bq, g_bp, g_b1, g_b2, g_table)])
    small = jnp.pad(small, (0, 256 * 128 - small.shape[0])).reshape(256, 128)
    return result, g_tok, gw_mlp, gw_att, small


ORDERS = (('core', 'x', 'y', 'z0', 'z1'), ('core', 'y', 'x', 'z0', 'z1'))
HALVES = (128, 64, 32, 16, 8)
LAND = (0, 128, 192, 224, 240)


def place():
    dp, sp = lax.axis_index('dp'), lax.axis_index('sp')
    bits = {'core': sp % 2, 'x': sp // 2, 'y': dp % 2, 'z0': (dp // 2) % 2, 'z1': dp // 4}
    unit = {'core': (0, 1), 'x': (0, 2), 'y': (1, 0), 'z0': (2, 0), 'z1': (4, 0)}
    peers = {k: (dp + (1 - 2 * b) * unit[k][0], sp + (1 - 2 * b) * unit[k][1]) for k, b in bits.items()}
    return bits, peers


class Stream:
    def __init__(self, order, ins, land, outs, send, recv):
        bits, self.peers = place()
        self.order, self.ins, self.land, self.outs, self.send, self.recv = order, ins, land, outs, send, recv
        self.bits = [bits[k] for k in order]
        offs = [0]
        for b, half in zip(self.bits, HALVES):
            offs.append(offs[-1] + b * half)
        self.offs = offs

    def rows(self, start, size):
        return pl.ds(pl.multiple_of(start, 8), size)

    def copy(self, k):
        j = k if k < 5 else 9 - k
        half = HALVES[j]
        if k == 0:
            src = self.ins.at[self.rows((1 - self.bits[0]) * half, half)]
        elif k < 5:
            src = self.land.at[self.rows(LAND[j - 1] + (1 - self.bits[j]) * half, half)]
        else:
            src = self.outs.at[self.rows(self.offs[j + 1], half)]
        dst = self.land.at[pl.ds(LAND[j], half)] if k < 5 else self.outs.at[self.rows(self.offs[j + 1], half)]
        return pltpu.make_async_remote_copy(src_ref=src, dst_ref=dst, send_sem=self.send.at[k], recv_sem=self.recv.at[k],
                                            device_id=self.peers[self.order[j]], device_id_type=pl.DeviceIdType.MESH)

    def finish(self, k):
        self.copy(k).wait()
        if k < 5:
            half = HALVES[k]
            if k == 0:
                kept = self.ins[self.rows(self.bits[0] * half, half), :]
            else:
                kept = self.land[self.rows(LAND[k - 1] + self.bits[k] * half, half), :]
            total = self.land[pl.ds(LAND[k], half), :] + kept
            if k < 4:
                self.land[pl.ds(LAND[k], half), :] = total
            else:
                self.outs[self.rows(self.offs[5], half), :] = total

    def advance(self, k):
        if k > 0:
            self.finish(k - 1)
        if k < 10:
            self.copy(k).start()


def reduce_kernel(*refs, counts):
    n = len(counts)
    ins, small_in = refs[:n], refs[n]
    outs, small_out = refs[n + 1:2 * n + 1], refs[2 * n + 1]
    land, small_land, send, recv, small_send, small_recv = refs[2 * n + 2:]
    peers = place()[1]
    barrier = pltpu.get_barrier_semaphore()
    for k in ORDERS[0]:
        pl.semaphore_signal(barrier, inc=1, device_id=peers[k], device_id_type=pl.DeviceIdType.MESH)
    pl.semaphore_wait(barrier, 5)
    base = 0
    slots = sum(counts) // 2
    groups = []
    for ref_in, ref_out, count in zip(ins, outs, counts):
        groups.append((base // 2, count // 2, ref_in, ref_out))
        base += count

    def tick(t, carry):
        for k in range(10, -1, -1):
            for first, length, ref_in, ref_out in groups:
                @pl.when((t - k >= first) & (t - k < first + length))
                def _():
                    u = t - k
                    for side in range(2):
                        s = 2 * u + side
                        i = s - 2 * first
                        Stream(ORDERS[side], ref_in.at[i], land.at[s], ref_out.at[i], send.at[s], recv.at[s]).advance(k)

            @pl.when(t == k)
            def _():
                Stream(ORDERS[0], small_in, small_land, small_out, small_send, small_recv).advance(k)
        return carry
    lax.fori_loop(0, slots + 10, tick, 0)


def reduce_all(arrays, small):
    counts = tuple(a.shape[0] for a in arrays)
    total = sum(counts)
    vmem = pl.BlockSpec(memory_space=pltpu.VMEM)
    outs = [sds(a.shape, F32) for a in arrays] + [sds(small.shape, F32)]
    return pl.pallas_call(
        functools.partial(reduce_kernel, counts=counts), in_specs=[vmem] * (len(arrays) + 1), out_specs=[vmem] * len(outs), out_shape=outs,
        scratch_shapes=[pltpu.VMEM((total, 248, 512), F32), pltpu.VMEM((248, 128), F32), pltpu.SemaphoreType.DMA((total, 10)),
                        pltpu.SemaphoreType.DMA((total, 10)), pltpu.SemaphoreType.DMA((10,)), pltpu.SemaphoreType.DMA((10,))],
        name="reduce", compiler_params=pltpu.CompilerParams(collective_id=0, has_side_effects=True, vmem_limit_bytes=VMEM_LIMIT))(*arrays, small)


def unpack(gw_mlp, gw_att, small, shapes):
    (s_nm, s_wr, s_na, s_wq, s_bq, s_table, s_wp, s_bp, s_nb, s_w1, s_b1, s_w2, s_b2) = shapes
    flat = small.reshape(-1)
    got, at = [], 0
    for shape in (s_nm, s_na, s_nb, s_bq, s_bp, s_b1, s_b2):
        size = math.prod(shape)
        got.append(flat[at:at + size].reshape(shape))
        at += size
    g_nm, g_na, g_nb, g_bq, g_bp, g_b1, g_b2 = got
    pad = -(-s_table[0] // 128) * 128
    g_table = flat[at:at + s_table[1] * pad].reshape(s_table[1], pad).T[:s_table[0]]
    wide = lambda x, shape: x.reshape(-1, shape[0], 512).transpose(1, 0, 2).reshape(shape)
    n1 = s_w1[1] // 256
    g_w1, g_w2 = wide(gw_mlp[:n1], s_w1), gw_mlp[n1:].reshape(s_w2)
    nr, nq = s_wr[0] // 256, s_wq[1] // 256
    g_wr, g_wq, g_wp = gw_att[:nr].reshape(s_wr), wide(gw_att[nr:nr + nq], s_wq), gw_att[nr + nq:].reshape(s_wp)
    return g_nm, g_wr, g_na, g_wq, g_bq, g_table, g_wp, g_bp, g_nb, g_w1, g_b1, g_w2, g_b2


def solution(mesh):
    def device_fn(tokens, grad_out, rel_index, *weights):
        nb = mesh.shape['sp']
        cot = lax.all_to_all(grad_out, 'sp', 1, 0, tiled=True)
        result, g_tok, gw_mlp, gw_att, small = local_step(tokens, cot, rel_index, weights)
        result = lax.all_to_all(result.reshape(cot.shape), 'sp', 0, 1, tiled=True)
        gw_mlp, gw_att, small = reduce_all([gw_mlp, gw_att], small)
        return (result, g_tok) + unpack(gw_mlp, gw_att, small, [w.shape for w in weights])

    rep_specs = (P(),) * 13
    return jax.shard_map(device_fn, mesh=mesh, in_specs=(P('dp', 'sp'), P(('dp', 'sp')), P()) + rep_specs, out_specs=(P(('dp', 'sp')), P('dp', 'sp')) + rep_specs, check_vma=False)
```

```python
import functools
import math
import numpy as np
import jax
import jax.numpy as jnp
from jax import lax
from jax.experimental import pallas as pl
from jax.experimental.pallas import tpu as pltpu
from jax.sharding import PartitionSpec as P

NORM_EPS = 1e-5
BF, F32 = jnp.bfloat16, jnp.float32
VMEM_LIMIT = 60 * 1024 * 1024
HEAD_GROUP = 8
GROUP_ROWS = 4


def dot_nn(a, b):
    return lax.dot_general(a, b, (((1,), (0,)), ((), ())), preferred_element_type=F32)


def dot_nt(a, b):
    return lax.dot_general(a, b, (((1,), (1,)), ((), ())), preferred_element_type=F32)


def dot_tn(a, b):
    return lax.dot_general(a, b, (((0,), (0,)), ((), ())), preferred_element_type=F32)


def norm_hat(x):
    mu = jnp.mean(x, axis=-1, keepdims=True)
    xc = x - mu
    rstd = lax.rsqrt(jnp.mean(xc * xc, axis=-1, keepdims=True) + NORM_EPS)
    return xc * rstd, rstd


def norm_fwd(x, norm_ref):
    hat, rstd = norm_hat(x)
    return hat * norm_ref[0:1, :].astype(F32) + norm_ref[1:2, :].astype(F32), hat, rstd


def norm_bwd(dy, hat, rstd, norm_ref):
    dhat = dy * norm_ref[0:1, :].astype(F32)
    m1 = jnp.mean(dhat, axis=-1, keepdims=True)
    m2 = jnp.mean(dhat * hat, axis=-1, keepdims=True)
    dx = rstd * (dhat - m1 - hat * m2)
    return dx, jnp.sum(dy * hat, axis=0, keepdims=True), jnp.sum(dy, axis=0, keepdims=True)


def head_masks(width, head_dim, dtype):
    lane = lax.broadcasted_iota(jnp.int32, (1, width), 1) // head_dim
    return [jnp.where(lane == h, 1.0, 0.0).astype(dtype) for h in range(width // head_dim)]


def stack_heads(x, masks):
    return jnp.concatenate([x * m for m in masks], axis=0)


def unstack_heads(x, masks, seq):
    total = x[0:seq] * masks[0]
    for h in range(1, len(masks)):
        total = total + x[h * seq:(h + 1) * seq] * masks[h]
    return total


def pos_kernel(table_ref, idx_ref, pos_ref):
    seq = idx_ref.shape[0]
    n_pieces = table_ref.shape[1] // 128
    for g in range(pos_ref.shape[0]):
        wide = jnp.concatenate([idx_ref[...]] * HEAD_GROUP, axis=1)
        for c in range(wide.shape[1] // 128):
            idx = wide[:, c * 128:(c + 1) * 128]
            low, high = idx & 127, idx >> 7
            lane = lax.broadcasted_iota(jnp.int32, idx.shape, 1) + c * 128
            out = jnp.zeros(idx.shape, F32)
            for h in range((c * 128) // seq, (c * 128 + 127) // seq + 1):
                val = jnp.zeros(idx.shape, F32)
                for t in range(n_pieces):
                    row = table_ref[g * HEAD_GROUP + h:g * HEAD_GROUP + h + 1, t * 128:(t + 1) * 128]
                    got = jnp.take_along_axis(jnp.broadcast_to(row, idx.shape), low, axis=1)
                    val = jnp.where(high == t, got, val)
                out = jnp.where((lane >= h * seq) & (lane < (h + 1) * seq), val, out)
            pos_ref[g, :, c * 128:(c + 1) * 128] = out


def fwd_kernel(tok_ref, perm_ref, pos_ref, nm_ref, wr_ref, na_ref, wq_ref, bq_ref, wp_ref, bp_ref,
               raw_ref, h0_ref, qkv_ref, att_ref, lse_ref, h1_ref, *, head_dim, seq):
    dim = h0_ref.shape[2]
    x = tok_ref[0].reshape(-1, tok_ref.shape[3])
    step = perm_ref.shape[0]
    quad = step // 4
    piece = quad // 2
    for g in range(x.shape[0] // step):
        y = dot_nn(perm_ref[...], x[g * step:(g + 1) * step])
        for w in range(2):
            cat = jnp.concatenate([y[p * quad + w * piece:p * quad + (w + 1) * piece] for p in range(4)], axis=1)
            raw_ref[0, w * seq + g * piece:w * seq + (g + 1) * piece, :] = cat.astype(BF)
    merged = norm_fwd(raw_ref[0].astype(F32), nm_ref)[0].astype(BF)
    h0 = dot_nn(merged, wr_ref[...]).astype(BF)
    h0_ref[0] = h0
    a = norm_fwd(h0.astype(F32), na_ref)[0].astype(BF)
    qkv_ref[0] = (dot_nn(a, wq_ref[...]) + bq_ref[...].astype(F32)).astype(BF)
    width = HEAD_GROUP * head_dim
    masks, masks_f = head_masks(width, head_dim, BF), head_masks(width, head_dim, F32)
    scale = head_dim ** -0.5
    for w in range(2):
        rows = slice(w * seq, (w + 1) * seq)
        for g in range(dim // width):
            cols = [slice(t * dim + g * width, t * dim + (g + 1) * width) for t in range(3)]
            q, k, v = (qkv_ref[0, rows, c] for c in cols)
            s = dot_nt(k, stack_heads(q, masks)) * scale + pos_ref[g]
            top = jnp.max(s, axis=0, keepdims=True)
            e = jnp.exp(s - top)
            den = jnp.sum(e, axis=0, keepdims=True)
            prob = (e * (1.0 / den)).astype(BF)
            lse_ref[0, w, g] = top + jnp.log(den)
            att_ref[0, rows, g * width:(g + 1) * width] = unstack_heads(dot_tn(prob, v), masks_f, seq).astype(BF)
    h1 = h0_ref[0].astype(F32) + dot_nn(att_ref[0], wp_ref[...]) + bp_ref[...].astype(F32)
    h1_ref[0] = h1.astype(BF)


def mlp_kernel(h1_ref, cot_ref, perm_ref, nb_ref, w1_ref, b1_ref, w2_ref, b2_ref,
               out_ref, dh1_ref, hid_ref, dpre_ref, b_ref, cotw_ref, gb1_ref, gb2_ref, gnb_ref):
    i = pl.program_id(0)

    @pl.when(i == 0)
    def _():
        gb1_ref[...] = jnp.zeros(gb1_ref.shape, F32)
        gb2_ref[...] = jnp.zeros(gb2_ref.shape, F32)
        gnb_ref[...] = jnp.zeros(gnb_ref.shape, F32)

    h1 = h1_ref[0].astype(F32)
    normed, hat, rstd = norm_fwd(h1, nb_ref)
    nb = normed.astype(BF)
    b_ref[0] = nb
    cot = dot_nn(perm_ref[...], cot_ref[0])
    cot_bf = cot.astype(BF)
    cotw_ref[0] = cot_bf
    gb2_ref[...] += jnp.sum(cot, axis=0, keepdims=True)
    out = h1 + b2_ref[...].astype(F32)
    d_norm = jnp.zeros(h1.shape, F32)
    chunk = 512
    for c in range(w1_ref.shape[1] // chunk):
        cols = slice(c * chunk, (c + 1) * chunk)
        pre = dot_nn(nb, w1_ref[:, cols]) + b1_ref[:, cols].astype(F32)
        phi = 0.5 + 0.5 * lax.erf(pre * math.sqrt(0.5))
        hid = (pre * phi).astype(BF)
        hid_ref[0, :, cols] = hid
        out = out + dot_nn(hid, w2_ref[cols, :])
        d_act = phi + pre * (jnp.exp(pre * pre * -0.5) * (1.0 / math.sqrt(2.0 * math.pi)))
        d_pre = dot_nt(cot_bf, w2_ref[cols, :]) * d_act
        gb1_ref[:, cols] += jnp.sum(d_pre, axis=0, keepdims=True)
        d_pre_bf = d_pre.astype(BF)
        dpre_ref[0, :, cols] = d_pre_bf
        d_norm = d_norm + dot_nt(d_pre_bf, w1_ref[:, cols])
    out_ref[0] = dot_tn(perm_ref[...], out.astype(BF)).astype(BF)
    dx, g_gain, g_shift = norm_bwd(d_norm, hat, rstd, nb_ref)
    gnb_ref[0:1, :] += g_gain
    gnb_ref[1:2, :] += g_shift
    dh1_ref[0] = cot + dx


def bwd_kernel(dh1_ref, raw_ref, h0_ref, qkv_ref, lse_ref, perm_ref, pos_ref, nm_ref, wr_ref, na_ref, wq_ref, wp_ref,
               gtok_ref, dh1b_ref, a_ref, dqkv_ref, m_ref, dh0_ref, gbp_ref, gbq_ref, gna_ref, gnm_ref, gpos_ref,
               datt_s, dqkv_f, *, head_dim, seq):
    i = pl.program_id(0)
    dim = h0_ref.shape[2]

    @pl.when(i == 0)
    def _():
        for ref in (gbp_ref, gbq_ref, gna_ref, gnm_ref, gpos_ref):
            ref[...] = jnp.zeros(ref.shape, F32)

    dh1 = dh1_ref[0]
    gbp_ref[...] += jnp.sum(dh1, axis=0, keepdims=True)
    dh1_bf = dh1.astype(BF)
    dh1b_ref[0] = dh1_bf
    datt_s[...] = dot_nt(dh1_bf, wp_ref[...]).astype(BF)
    width = HEAD_GROUP * head_dim
    masks, masks_f = head_masks(width, head_dim, BF), head_masks(width, head_dim, F32)
    scale = head_dim ** -0.5
    for w in range(2):
        rows = slice(w * seq, (w + 1) * seq)
        for g in range(dim // width):
            cols = [slice(t * dim + g * width, t * dim + (g + 1) * width) for t in range(3)]
            q, k, v = (qkv_ref[0, rows, c] for c in cols)
            qm = stack_heads(q, masks)
            dam = stack_heads(datt_s[rows, g * width:(g + 1) * width], masks)
            prob = jnp.exp(dot_nt(k, qm) * scale + pos_ref[g] - lse_ref[0, w, g])
            d_prob = dot_nt(v, dam)
            dqkv_f[rows, cols[2]] = dot_nn(prob.astype(BF), dam)
            delta = jnp.sum(d_prob * prob, axis=0, keepdims=True)
            ds = prob * (d_prob - delta)
            gpos_ref[g] += ds
            ds_bf = (ds * scale).astype(BF)
            dqkv_f[rows, cols[1]] = dot_nn(ds_bf, qm)
            dqkv_f[rows, cols[0]] = unstack_heads(dot_tn(ds_bf, k), masks_f, seq)
    gbq_ref[...] += jnp.sum(dqkv_f[...], axis=0, keepdims=True)
    dqkv_bf = dqkv_f[...].astype(BF)
    dqkv_ref[0] = dqkv_bf
    d_a = dot_nt(dqkv_bf, wq_ref[...])
    normed, hat, rstd = norm_fwd(h0_ref[0].astype(F32), na_ref)
    a_ref[0] = normed.astype(BF)
    dx, g_gain, g_shift = norm_bwd(d_a, hat, rstd, na_ref)
    gna_ref[0:1, :] += g_gain
    gna_ref[1:2, :] += g_shift
    dh0_bf = (dh1 + dx).astype(BF)
    dh0_ref[0] = dh0_bf
    d_m = dot_nt(dh0_bf, wr_ref[...])
    normed, hat, rstd = norm_fwd(raw_ref[0].astype(F32), nm_ref)
    m_ref[0] = normed.astype(BF)
    dx, g_gain, g_shift = norm_bwd(d_m, hat, rstd, nm_ref)
    gnm_ref[0:1, :] += g_gain
    gnm_ref[1:2, :] += g_shift
    d_raw = dx.astype(BF)
    step = perm_ref.shape[0]
    quad = step // 4
    piece = quad // 2
    chan = d_raw.shape[1] // 4
    tok_rows = step // gtok_ref.shape[2]
    for g in range(seq // piece):
        y = jnp.concatenate([d_raw[w * seq + g * piece:w * seq + (g + 1) * piece, p * chan:(p + 1) * chan]
                             for p in range(4) for w in range(2)], axis=0)
        gtok_ref[0, g * tok_rows:(g + 1) * tok_rows] = dot_tn(perm_ref[...], y).astype(BF).reshape(tok_rows, gtok_ref.shape[2], chan)


def whole(shape):
    zeros = (0,) * len(shape)
    return pl.BlockSpec(shape, lambda i: zeros, pipeline_mode=pl.Buffered(1))


def out_whole(shape):
    zeros = (0,) * len(shape)
    return pl.BlockSpec(shape, lambda i: zeros)


def band(shape):
    zeros = (0,) * (len(shape) - 1)
    return pl.BlockSpec((1,) + shape[1:], lambda i: (i,) + zeros)


def sds(shape, dtype):
    return jax.ShapeDtypeStruct(shape, dtype)


def call(kernel, grid, ins, in_specs, outs, out_specs, scratch, flops, name):
    moved = sum(math.prod(a.shape) * a.dtype.itemsize for a in list(ins) + list(outs))
    return pl.pallas_call(
        kernel, grid=grid, in_specs=in_specs, out_specs=out_specs, out_shape=outs, scratch_shapes=scratch, name=name,
        cost_estimate=pl.CostEstimate(flops=flops, bytes_accessed=moved, transcendentals=0),
        compiler_params=pltpu.CompilerParams(vmem_limit_bytes=VMEM_LIMIT, dimension_semantics=("arbitrary",) * len(grid)))(*ins)


def merge_perm(window, cols):
    rows_in = 2 * GROUP_ROWS * cols
    perm = np.zeros((rows_in, rows_in), np.float32)
    out = 0
    for quad in range(4):
        c, r = quad // 2, quad % 2
        for w in range(2):
            for i in range(GROUP_ROWS):
                for j in range(window):
                    perm[out, (2 * i + r) * cols + 2 * (w * window + j) + c] = 1.0
                    out += 1
    return jnp.asarray(perm, BF)


def window_perm(window):
    n = 2 * window * window
    perm = np.zeros((n, n), np.float32)
    for w in range(2):
        for i in range(window):
            for j in range(window):
                perm[(w * window + i) * window + j, (i * 2 + w) * window + j] = 1.0
    return jnp.asarray(perm, BF)


def local_step(tokens, cot, rel_index, weights):
    (norm_merge, w_reduce, norm_attn, w_qkv, b_qkv, rel_table, w_proj, b_proj, norm_mlp, w_fc1, b_fc1, w_fc2, b_fc2) = weights
    nb, tok_rows, tok_cols, chan = tokens.shape
    dim = w_reduce.shape[1]
    ff = w_fc1.shape[1]
    n_heads = rel_table.shape[1]
    head_dim = dim // n_heads
    seq = rel_index.shape[0]
    window = math.isqrt(seq)
    n = 2 * seq
    groups = n_heads // HEAD_GROUP
    lanes = HEAD_GROUP * seq
    table_pad = -(-rel_table.shape[0] // 128) * 128
    perm4, perm_w = merge_perm(window, tok_cols), window_perm(window)
    table_t = jnp.pad(rel_table.astype(F32).T, ((0, 0), (0, table_pad - rel_table.shape[0])))
    idx_t = rel_index.T
    row = lambda x: x.reshape(1, -1)

    pos = call(pos_kernel, (1,), (table_t, idx_t), [whole(table_t.shape), whole(idx_t.shape)],
               [sds((groups, seq, lanes), F32)], [out_whole((groups, seq, lanes))], [], 10**7, "pos")[0]

    ins = (tokens, perm4, pos, norm_merge, w_reduce, norm_attn, w_qkv, row(b_qkv), w_proj, row(b_proj))
    outs = [sds((nb, n, 4 * chan), BF), sds((nb, n, dim), BF), sds((nb, n, 3 * dim), BF), sds((nb, n, dim), BF),
            sds((nb, 2, groups, 1, lanes), F32), sds((nb, n, dim), BF)]
    raw, h0, qkv, att, lse, h1 = call(
        functools.partial(fwd_kernel, head_dim=head_dim, seq=seq), (nb,), ins,
        [band(tokens.shape)] + [whole(a.shape) for a in ins[1:]], outs, [band(o.shape) for o in outs], [], 8 * 10**9, "fwd")

    ins = (h1, cot.reshape(nb, n, dim), perm_w, norm_mlp, w_fc1, row(b_fc1), w_fc2, row(b_fc2))
    tok = lambda width, dtype=BF: sds((nb, n, width), dtype)
    outs = [tok(dim), tok(dim, F32), tok(ff), tok(ff), tok(dim), tok(dim), sds((1, ff), F32), sds((1, dim), F32), sds((2, dim), F32)]
    result, dh1, hid, dpre, b_in, cot_w, g_b1, g_b2, g_nb = call(
        mlp_kernel, (nb,), ins, [band(ins[0].shape), band(ins[1].shape)] + [whole(a.shape) for a in ins[2:]],
        outs, [band(o.shape) for o in outs[:6]] + [out_whole(o.shape) for o in outs[6:]], [], 12 * 10**9, "mlp")

    ins = (dh1, raw, h0, qkv, lse, perm4, pos, norm_merge, w_reduce, norm_attn, w_qkv, w_proj)
    outs = [sds(tokens.shape, BF), tok(dim), tok(dim), tok(3 * dim), tok(4 * chan), tok(dim), sds((1, dim), F32),
            sds((1, 3 * dim), F32), sds((2, dim), F32), sds((2, 4 * chan), F32), sds((groups, seq, lanes), F32)]
    g_tok, dh1_bf, a_in, dqkv, m_in, dh0, g_bp, g_bq, g_na, g_nm, g_pos = call(
        functools.partial(bwd_kernel, head_dim=head_dim, seq=seq), (nb,), ins,
        [band(a.shape) for a in ins[:5]] + [whole(a.shape) for a in ins[5:]],
        outs, [band(o.shape) for o in outs[:6]] + [out_whole(o.shape) for o in outs[6:]],
        [pltpu.VMEM((n, dim), BF), pltpu.VMEM((n, 3 * dim), F32)], 12 * 10**9, "bwd")

    small = jnp.concatenate([x.reshape(-1) for x in (g_nm, g_na, g_nb, g_bq, g_bp, g_b1, g_b2)])
    room = 256 - n_heads * table_pad // 128
    small = jnp.pad(small, (0, room * 128 - small.shape[0])).reshape(room, 128)
    pairs = [(hid, cot_w), (b_in, dpre), (m_in, dh0), (a_in, dqkv), (att, dh1_bf)]
    return result, g_tok, [tuple(x.reshape(nb * n, -1) for x in pair) for pair in pairs], small, g_pos, idx_t


ORDERS = (('core', 'x', 'y', 'z0', 'z1'), ('core', 'y', 'x', 'z0', 'z1'), ('core', 'z0', 'z1', 'x', 'y'), ('core', 'z0', 'z1', 'y', 'x'))
HALVES = (128, 64, 32, 16, 8)
LAND = (0, 128, 192, 224, 240)
WIDTH = 512
STARTS = tuple(range(1, 23, 2))
Z_FIRST = 5
TABLE_STEP = 8


def place():
    dp, sp = lax.axis_index('dp'), lax.axis_index('sp')
    bits = {'core': sp % 2, 'x': sp // 2, 'y': dp % 2, 'z0': (dp // 2) % 2, 'z1': dp // 4}
    unit = {'core': (0, 1), 'x': (0, 2), 'y': (1, 0), 'z0': (2, 0), 'z1': (4, 0)}
    peers = {k: (dp + (1 - 2 * b) * unit[k][0], sp + (1 - 2 * b) * unit[k][1]) for k, b in bits.items()}
    return bits, peers


class Stream:
    def __init__(self, order, other, swap, buf, land, send, recv):
        bits, peers = place()
        pick = lambda a, b: a if a is b else jnp.where(swap, b, a)
        self.buf, self.land, self.send, self.recv = buf, land, send, recv
        self.bits = [pick(bits[a], bits[b]) for a, b in zip(order, other)]
        self.peers = [tuple(pick(p, q) for p, q in zip(peers[a], peers[b])) for a, b in zip(order, other)]
        offs = [0]
        for b, half in zip(self.bits, HALVES):
            offs.append(offs[-1] + b * half)
        self.offs = offs

    def rows(self, start, size):
        return pl.ds(pl.multiple_of(start, 8), size)

    def copy(self, k):
        j = k if k < 5 else 9 - k
        half = HALVES[j]
        if k == 0:
            src = self.buf.at[self.rows((1 - self.bits[0]) * half, half)]
        elif k < 5:
            src = self.land.at[self.rows(LAND[j - 1] + (1 - self.bits[j]) * half, half)]
        else:
            src = self.buf.at[self.rows(self.offs[j + 1], half)]
        dst = self.land.at[pl.ds(LAND[j], half)] if k < 5 else self.buf.at[self.rows(self.offs[j + 1], half)]
        return pltpu.make_async_remote_copy(src_ref=src, dst_ref=dst, send_sem=self.send.at[k], recv_sem=self.recv.at[k],
                                            device_id=self.peers[j], device_id_type=pl.DeviceIdType.MESH)

    def finish(self, k):
        self.copy(k).wait()
        if k < 5:
            half = HALVES[k]
            if k == 0:
                kept = self.buf[self.rows(self.bits[0] * half, half), :]
            else:
                kept = self.land[self.rows(LAND[k - 1] + self.bits[k] * half, half), :]
            total = self.land[pl.ds(LAND[k], half), :] + kept
            if k < 4:
                self.land[pl.ds(LAND[k], half), :] = total
            else:
                self.buf[self.rows(self.offs[5], half), :] = total

    def advance(self, k):
        if k > 0:
            self.finish(k - 1)
        if k < 10:
            self.copy(k).start()


def add_table(pos_s, idx_ref, table_s, first):
    row = lax.broadcasted_iota(jnp.int32, (table_s.shape[1], idx_ref.shape[1]), 0)
    acc = table_s[...]
    for j in range(TABLE_STEP):
        m = first + j
        hot = jnp.where(row == idx_ref[pl.ds(m, 1), :], 1.0, 0.0).astype(BF)
        val = pos_s[m]
        hi = val.astype(BF)
        rest = val - hi.astype(F32)
        mid = rest.astype(BF)
        low = (rest - mid.astype(F32)).astype(BF)
        acc = acc + dot_nt(jnp.concatenate([hi, mid, low], axis=0), hot)
    table_s[...] = acc


def reduce_kernel(*refs, n):
    pairs, (small_in, gpos_ref, idx_ref) = refs[:2 * n], refs[2 * n:2 * n + 3]
    outs, small_out = refs[2 * n + 3:3 * n + 3], refs[3 * n + 3]
    held = refs[3 * n + 4:5 * n + 4]
    buf, land, small_land, pos_s, table_s, send, recv, small_send, small_recv, sem_in, sem_out = refs[5 * n + 4:]
    seq = idx_ref.shape[0]
    n_heads = pos_s.shape[1]
    total = buf.shape[0]
    loads = [pltpu.make_async_copy(a, b, sem_in.at[i]) for i, (a, b) in enumerate(zip(pairs, held))]
    for load in loads:
        load.start()
    groups, base = [], 0
    for i, out in enumerate(outs):
        count = out.shape[0] * out.shape[1] // (512 * WIDTH)
        groups.append((base, count, held[2 * i], held[2 * i + 1], out, loads[2 * i:2 * i + 2]))
        base += count

    def block(out, j, side):
        wide = out.shape[1] // WIDTH
        row0, col0 = j // wide * 512 + side * 256, j % wide * WIDTH
        return out.at[pl.ds(pl.multiple_of(row0, 256), 256), pl.ds(pl.multiple_of(col0, WIDTH), WIDTH)]

    def part(ref, j):
        return ref[...] if ref.shape[1] == WIDTH else ref[:, pl.ds(pl.multiple_of(j * WIDTH, WIDTH), WIDTH)]

    peers = place()[1]
    barrier = pltpu.get_barrier_semaphore()
    for k in ORDERS[0]:
        pl.semaphore_signal(barrier, inc=1, device_id=peers[k], device_id_type=pl.DeviceIdType.MESH)
    pl.semaphore_wait(barrier, 5)
    table_s[...] = jnp.zeros(table_s.shape, F32)
    room = small_in.shape[0]
    small_out[0:room, :] = small_in[...]
    table_ticks = seq // TABLE_STEP
    small_at = table_ticks + 2
    slots = total // 2

    def tick(t, carry):
        for k in range(10, -1, -1):
            u = t - STARTS[k]

            @pl.when((u >= 0) & (u < slots))
            def _():
                swap = lax.rem(u, Z_FIRST) == Z_FIRST - 1
                for side in range(2):
                    s = 2 * u + side
                    Stream(ORDERS[side], ORDERS[2 + side], swap, buf.at[s], land.at[s], send.at[s], recv.at[s]).advance(k)
                if k == 10:
                    for first, count, left, right, out, loads in groups:
                        @pl.when((u >= first) & (u < first + count))
                        def _():
                            for side in range(2):
                                s = 2 * u + side
                                pltpu.make_async_copy(buf.at[s], block(out, u - first, side), sem_out.at[s]).start()

            @pl.when(t == small_at + k)
            def _():
                Stream(ORDERS[0], ORDERS[0], None, small_out, small_land, small_send, small_recv).advance(k)

        for first, count, left, right, out, loads in groups:
            @pl.when(t == first)
            def _():
                for load in loads:
                    load.wait()

            @pl.when((t >= first) & (t < first + count))
            def _():
                value = dot_tn(part(left, t - first), part(right, t - first))
                buf[2 * t] = value[:256]
                buf[2 * t + 1] = value[256:]

        @pl.when(t == 0)
        def _():
            for g in range(gpos_ref.shape[0]):
                for h in range(HEAD_GROUP):
                    pos_s[:, g * HEAD_GROUP + h, :] = gpos_ref[g, :, h * seq:(h + 1) * seq]

        @pl.when((t >= 1) & (t < 1 + table_ticks))
        def _():
            add_table(pos_s, idx_ref, table_s, (t - 1) * TABLE_STEP)

        @pl.when(t == 1 + table_ticks)
        def _():
            summed = table_s[0:n_heads] + table_s[n_heads:2 * n_heads] + table_s[2 * n_heads:3 * n_heads]
            for p in range(table_s.shape[1] // 128):
                small_out[room + p * n_heads:room + (p + 1) * n_heads, :] = summed[:, p * 128:(p + 1) * 128]
        return carry
    lax.fori_loop(0, max(slots + STARTS[10] + 1, small_at + 11), tick, 0)

    def drain(s, carry):
        pltpu.make_async_copy(buf.at[s], block(outs[0], 0, 0), sem_out.at[s]).wait()
        return carry
    lax.fori_loop(0, total, drain, 0)


def reduce_all(pairs, small, g_pos, idx_t, n_heads):
    shapes = [(a.shape[1], b.shape[1]) for a, b in pairs]
    total = sum(a * b // (256 * WIDTH) for a, b in shapes)
    n = len(pairs)
    flat = [x for pair in pairs for x in pair]
    seq = idx_t.shape[0]
    table_pad = (256 - small.shape[0]) * 128 // n_heads
    vmem, hbm = pl.BlockSpec(memory_space=pltpu.VMEM), pl.BlockSpec(memory_space=pl.ANY)
    outs = [sds(shape, F32) for shape in shapes] + [sds((256, 128), F32)]
    dma = pltpu.SemaphoreType.DMA
    return pl.pallas_call(
        functools.partial(reduce_kernel, n=n), in_specs=[hbm] * (2 * n) + [vmem] * 3, out_specs=[hbm] * n + [vmem], out_shape=outs,
        scratch_shapes=[pltpu.VMEM(x.shape, x.dtype) for x in flat] + [
            pltpu.VMEM((total, 256, WIDTH), F32), pltpu.VMEM((total, 248, WIDTH), F32), pltpu.VMEM((248, 128), F32), pltpu.VMEM((seq, n_heads, seq), F32),
            pltpu.VMEM((3 * n_heads, table_pad), F32), dma((total, 10)), dma((total, 10)), dma((10,)), dma((10,)), dma((2 * n,)), dma((total,))],
        name="reduce", compiler_params=pltpu.CompilerParams(collective_id=0, has_side_effects=True, vmem_limit_bytes=63 * 1024 * 1024))(*flat, small, g_pos, idx_t)


def unpack_small(small, shapes):
    (s_nm, s_wr, s_na, s_wq, s_bq, s_table, s_wp, s_bp, s_nb, s_w1, s_b1, s_w2, s_b2) = shapes
    flat = small.reshape(-1)
    got, at = [], 0
    for shape in (s_nm, s_na, s_nb, s_bq, s_bp, s_b1, s_b2):
        size = math.prod(shape)
        got.append(flat[at:at + size].reshape(shape))
        at += size
    pad = -(-s_table[0] // 128) * 128
    rows = s_table[1] * pad // 128
    g_table = small[256 - rows:].reshape(pad // 128, s_table[1], 128).transpose(0, 2, 1).reshape(pad, s_table[1])[:s_table[0]]
    return got + [g_table]


def solution(mesh):
    def device_fn(tokens, grad_out, rel_index, *weights):
        nb = mesh.shape['sp']
        cot = lax.all_to_all(grad_out, 'sp', 1, 0, tiled=True)
        result, g_tok, grads, small, g_pos, idx_t = local_step(tokens, cot, rel_index, weights)
        result = lax.all_to_all(result.reshape(cot.shape), 'sp', 0, 1, tiled=True)
        g_w2, g_w1, g_wr, g_wq, g_wp, small = reduce_all(grads, small, g_pos, idx_t, weights[5].shape[1])
        g_nm, g_na, g_nb, g_bq, g_bp, g_b1, g_b2, g_table = unpack_small(small, [w.shape for w in weights])
        return result, g_tok, g_nm, g_wr, g_na, g_wq, g_bq, g_table, g_wp, g_bp, g_nb, g_w1, g_b1, g_w2, g_b2

    rep_specs = (P(),) * 13
    return jax.shard_map(device_fn, mesh=mesh, in_specs=(P('dp', 'sp'), P(('dp', 'sp')), P()) + rep_specs, out_specs=(P(('dp', 'sp')), P('dp', 'sp')) + rep_specs, check_vma=False)
```

```python
import functools
import math
import numpy as np
import jax
import jax.numpy as jnp
from jax import lax
from jax.experimental import pallas as pl
from jax.experimental.pallas import tpu as pltpu
from jax.sharding import PartitionSpec as P

NORM_EPS = 1e-5
BF, F32 = jnp.bfloat16, jnp.float32
VMEM_LIMIT = 60 * 1024 * 1024
HEAD_GROUP = 8
GROUP_ROWS = 4


def dot_nn(a, b):
    return lax.dot_general(a, b, (((1,), (0,)), ((), ())), preferred_element_type=F32)


def dot_nt(a, b):
    return lax.dot_general(a, b, (((1,), (1,)), ((), ())), preferred_element_type=F32)


def dot_tn(a, b):
    return lax.dot_general(a, b, (((0,), (0,)), ((), ())), preferred_element_type=F32)


def norm_hat(x):
    mu = jnp.mean(x, axis=-1, keepdims=True)
    xc = x - mu
    rstd = lax.rsqrt(jnp.mean(xc * xc, axis=-1, keepdims=True) + NORM_EPS)
    return xc * rstd, rstd


def norm_fwd(x, norm_ref):
    hat, rstd = norm_hat(x)
    return hat * norm_ref[0:1, :].astype(F32) + norm_ref[1:2, :].astype(F32), hat, rstd


def norm_bwd(dy, hat, rstd, norm_ref):
    dhat = dy * norm_ref[0:1, :].astype(F32)
    m1 = jnp.mean(dhat, axis=-1, keepdims=True)
    m2 = jnp.mean(dhat * hat, axis=-1, keepdims=True)
    dx = rstd * (dhat - m1 - hat * m2)
    return dx, jnp.sum(dy * hat, axis=0, keepdims=True), jnp.sum(dy, axis=0, keepdims=True)


def head_masks(width, head_dim, dtype):
    lane = lax.broadcasted_iota(jnp.int32, (1, width), 1) // head_dim
    return [jnp.where(lane == h, 1.0, 0.0).astype(dtype) for h in range(width // head_dim)]


def stack_heads(x, masks):
    return jnp.concatenate([x * m for m in masks], axis=0)


def unstack_heads(x, masks, seq):
    total = x[0:seq] * masks[0]
    for h in range(1, len(masks)):
        total = total + x[h * seq:(h + 1) * seq] * masks[h]
    return total


def pos_kernel(table_ref, idx_ref, pos_ref):
    seq = idx_ref.shape[0]
    n_pieces = table_ref.shape[1] // 128
    for g in range(pos_ref.shape[0]):
        wide = jnp.concatenate([idx_ref[...].T] * HEAD_GROUP, axis=1)
        for c in range(wide.shape[1] // 128):
            idx = wide[:, c * 128:(c + 1) * 128]
            low, high = idx & 127, idx >> 7
            lane = lax.broadcasted_iota(jnp.int32, idx.shape, 1) + c * 128
            out = jnp.zeros(idx.shape, F32)
            for h in range((c * 128) // seq, (c * 128 + 127) // seq + 1):
                val = jnp.zeros(idx.shape, F32)
                for t in range(n_pieces):
                    row = table_ref[g * HEAD_GROUP + h:g * HEAD_GROUP + h + 1, t * 128:(t + 1) * 128]
                    got = jnp.take_along_axis(jnp.broadcast_to(row, idx.shape), low, axis=1)
                    val = jnp.where(high == t, got, val)
                out = jnp.where((lane >= h * seq) & (lane < (h + 1) * seq), val, out)
            pos_ref[g, :, c * 128:(c + 1) * 128] = out


def fwd_kernel(tok_ref, perm_ref, pos_ref, nm_ref, wr_ref, na_ref, wq_ref, bq_ref, wp_ref, bp_ref,
               raw_ref, h0_ref, qkv_ref, att_ref, lse_ref, h1_ref, *, head_dim, seq):
    dim = h0_ref.shape[2]
    x = tok_ref[0].reshape(-1, tok_ref.shape[3])
    step = perm_ref.shape[0]
    quad = step // 4
    piece = quad // 2
    for g in range(x.shape[0] // step):
        y = dot_nn(perm_ref[...], x[g * step:(g + 1) * step])
        for w in range(2):
            cat = jnp.concatenate([y[p * quad + w * piece:p * quad + (w + 1) * piece] for p in range(4)], axis=1)
            raw_ref[0, w * seq + g * piece:w * seq + (g + 1) * piece, :] = cat.astype(BF)
    merged = norm_fwd(raw_ref[0].astype(F32), nm_ref)[0].astype(BF)
    h0 = dot_nn(merged, wr_ref[...]).astype(BF)
    h0_ref[0] = h0
    a = norm_fwd(h0.astype(F32), na_ref)[0].astype(BF)
    qkv_ref[0] = (dot_nn(a, wq_ref[...]) + bq_ref[...].astype(F32).reshape(1, -1)).astype(BF)
    width = HEAD_GROUP * head_dim
    masks, masks_f = head_masks(width, head_dim, BF), head_masks(width, head_dim, F32)
    scale = head_dim ** -0.5
    for w in range(2):
        rows = slice(w * seq, (w + 1) * seq)
        for g in range(dim // width):
            cols = [slice(t * dim + g * width, t * dim + (g + 1) * width) for t in range(3)]
            q, k, v = (qkv_ref[0, rows, c] for c in cols)
            s = dot_nt(k, stack_heads(q, masks)) * scale + pos_ref[g]
            top = jnp.max(s, axis=0, keepdims=True)
            e = jnp.exp(s - top)
            den = jnp.sum(e, axis=0, keepdims=True)
            prob = (e * (1.0 / den)).astype(BF)
            lse_ref[0, w, g] = top + jnp.log(den)
            att_ref[0, rows, g * width:(g + 1) * width] = unstack_heads(dot_tn(prob, v), masks_f, seq).astype(BF)
    h1 = h0_ref[0].astype(F32) + dot_nn(att_ref[0], wp_ref[...]) + bp_ref[...].astype(F32).reshape(1, -1)
    h1_ref[0] = h1.astype(BF)


def mlp_kernel(h1_ref, cot_ref, perm_ref, nb_ref, w1_ref, b1_ref, w2_ref, b2_ref,
               out_ref, dh1_ref, hid_ref, dpre_ref, b_ref, cotw_ref, gb1_ref, gb2_ref, gnb_ref):
    i = pl.program_id(0)

    @pl.when(i == 0)
    def _():
        gb1_ref[...] = jnp.zeros(gb1_ref.shape, F32)
        gb2_ref[...] = jnp.zeros(gb2_ref.shape, F32)
        gnb_ref[...] = jnp.zeros(gnb_ref.shape, F32)

    h1 = h1_ref[0].astype(F32)
    normed, hat, rstd = norm_fwd(h1, nb_ref)
    nb = normed.astype(BF)
    b_ref[0] = nb
    cot = dot_nn(perm_ref[...], cot_ref[0])
    cot_bf = cot.astype(BF)
    cotw_ref[0] = cot_bf
    gb2_ref[...] += jnp.sum(cot, axis=0, keepdims=True)
    out = h1 + b2_ref[...].astype(F32).reshape(1, -1)
    d_norm = jnp.zeros(h1.shape, F32)
    chunk = 512
    for c in range(w1_ref.shape[1] // chunk):
        cols = slice(c * chunk, (c + 1) * chunk)
        pre = dot_nn(nb, w1_ref[:, cols]) + b1_ref[cols].astype(F32).reshape(1, -1)
        phi = 0.5 + 0.5 * lax.erf(pre * math.sqrt(0.5))
        hid = (pre * phi).astype(BF)
        hid_ref[0, :, cols] = hid
        out = out + dot_nn(hid, w2_ref[cols, :])
        d_act = phi + pre * (jnp.exp(pre * pre * -0.5) * (1.0 / math.sqrt(2.0 * math.pi)))
        d_pre = dot_nt(cot_bf, w2_ref[cols, :]) * d_act
        gb1_ref[:, cols] += jnp.sum(d_pre, axis=0, keepdims=True)
        d_pre_bf = d_pre.astype(BF)
        dpre_ref[0, :, cols] = d_pre_bf
        d_norm = d_norm + dot_nt(d_pre_bf, w1_ref[:, cols])
    out_ref[0] = dot_tn(perm_ref[...], out.astype(BF)).astype(BF)
    dx, g_gain, g_shift = norm_bwd(d_norm, hat, rstd, nb_ref)
    gnb_ref[0:1, :] += g_gain
    gnb_ref[1:2, :] += g_shift
    dh1_ref[0] = cot + dx


def bwd_kernel(dh1_ref, raw_ref, h0_ref, qkv_ref, lse_ref, perm_ref, pos_ref, nm_ref, wr_ref, na_ref, wq_ref, wp_ref,
               gtok_ref, dh1b_ref, a_ref, dqkv_ref, m_ref, dh0_ref, gbp_ref, gbq_ref, gna_ref, gnm_ref, gpos_ref,
               datt_s, dqkv_f, *, head_dim, seq):
    i = pl.program_id(0)
    dim = h0_ref.shape[2]

    @pl.when(i == 0)
    def _():
        for ref in (gbp_ref, gbq_ref, gna_ref, gnm_ref, gpos_ref):
            ref[...] = jnp.zeros(ref.shape, F32)

    dh1 = dh1_ref[0]
    gbp_ref[...] += jnp.sum(dh1, axis=0, keepdims=True)
    dh1_bf = dh1.astype(BF)
    dh1b_ref[0] = dh1_bf
    datt_s[...] = dot_nt(dh1_bf, wp_ref[...]).astype(BF)
    width = HEAD_GROUP * head_dim
    masks, masks_f = head_masks(width, head_dim, BF), head_masks(width, head_dim, F32)
    scale = head_dim ** -0.5
    for w in range(2):
        rows = slice(w * seq, (w + 1) * seq)
        for g in range(dim // width):
            cols = [slice(t * dim + g * width, t * dim + (g + 1) * width) for t in range(3)]
            q, k, v = (qkv_ref[0, rows, c] for c in cols)
            qm = stack_heads(q, masks)
            dam = stack_heads(datt_s[rows, g * width:(g + 1) * width], masks)
            prob = jnp.exp(dot_nt(k, qm) * scale + pos_ref[g] - lse_ref[0, w, g])
            d_prob = dot_nt(v, dam)
            dqkv_f[rows, cols[2]] = dot_nn(prob.astype(BF), dam)
            delta = jnp.sum(d_prob * prob, axis=0, keepdims=True)
            ds = prob * (d_prob - delta)
            gpos_ref[g] += ds
            ds_bf = (ds * scale).astype(BF)
            dqkv_f[rows, cols[1]] = dot_nn(ds_bf, qm)
            dqkv_f[rows, cols[0]] = unstack_heads(dot_tn(ds_bf, k), masks_f, seq)
    gbq_ref[...] += jnp.sum(dqkv_f[...], axis=0, keepdims=True)
    dqkv_bf = dqkv_f[...].astype(BF)
    dqkv_ref[0] = dqkv_bf
    d_a = dot_nt(dqkv_bf, wq_ref[...])
    normed, hat, rstd = norm_fwd(h0_ref[0].astype(F32), na_ref)
    a_ref[0] = normed.astype(BF)
    dx, g_gain, g_shift = norm_bwd(d_a, hat, rstd, na_ref)
    gna_ref[0:1, :] += g_gain
    gna_ref[1:2, :] += g_shift
    dh0_bf = (dh1 + dx).astype(BF)
    dh0_ref[0] = dh0_bf
    d_m = dot_nt(dh0_bf, wr_ref[...])
    normed, hat, rstd = norm_fwd(raw_ref[0].astype(F32), nm_ref)
    m_ref[0] = normed.astype(BF)
    dx, g_gain, g_shift = norm_bwd(d_m, hat, rstd, nm_ref)
    gnm_ref[0:1, :] += g_gain
    gnm_ref[1:2, :] += g_shift
    d_raw = dx.astype(BF)
    step = perm_ref.shape[0]
    quad = step // 4
    piece = quad // 2
    chan = d_raw.shape[1] // 4
    tok_rows = step // gtok_ref.shape[2]
    for g in range(seq // piece):
        y = jnp.concatenate([d_raw[w * seq + g * piece:w * seq + (g + 1) * piece, p * chan:(p + 1) * chan]
                             for p in range(4) for w in range(2)], axis=0)
        gtok_ref[0, g * tok_rows:(g + 1) * tok_rows] = dot_tn(perm_ref[...], y).astype(BF).reshape(tok_rows, gtok_ref.shape[2], chan)


def whole(shape):
    zeros = (0,) * len(shape)
    return pl.BlockSpec(shape, lambda i: zeros, pipeline_mode=pl.Buffered(1))


def out_whole(shape):
    zeros = (0,) * len(shape)
    return pl.BlockSpec(shape, lambda i: zeros)


def band(shape):
    zeros = (0,) * (len(shape) - 1)
    return pl.BlockSpec((1,) + shape[1:], lambda i: (i,) + zeros)


def sds(shape, dtype):
    return jax.ShapeDtypeStruct(shape, dtype)


def call(kernel, grid, ins, in_specs, outs, out_specs, scratch, flops, name):
    moved = sum(math.prod(a.shape) * a.dtype.itemsize for a in list(ins) + list(outs))
    return pl.pallas_call(
        kernel, grid=grid, in_specs=in_specs, out_specs=out_specs, out_shape=outs, scratch_shapes=scratch, name=name,
        cost_estimate=pl.CostEstimate(flops=flops, bytes_accessed=moved, transcendentals=0),
        compiler_params=pltpu.CompilerParams(vmem_limit_bytes=VMEM_LIMIT, dimension_semantics=("arbitrary",) * len(grid)))(*ins)


def merge_perm(window, cols):
    rows_in = 2 * GROUP_ROWS * cols
    perm = np.zeros((rows_in, rows_in), np.float32)
    out = 0
    for quad in range(4):
        c, r = quad // 2, quad % 2
        for w in range(2):
            for i in range(GROUP_ROWS):
                for j in range(window):
                    perm[out, (2 * i + r) * cols + 2 * (w * window + j) + c] = 1.0
                    out += 1
    return jnp.asarray(perm, BF)


def window_perm(window):
    n = 2 * window * window
    perm = np.zeros((n, n), np.float32)
    for w in range(2):
        for i in range(window):
            for j in range(window):
                perm[(w * window + i) * window + j, (i * 2 + w) * window + j] = 1.0
    return jnp.asarray(perm, BF)


def local_step(tokens, cot, rel_index, weights):
    (norm_merge, w_reduce, norm_attn, w_qkv, b_qkv, rel_table, w_proj, b_proj, norm_mlp, w_fc1, b_fc1, w_fc2, b_fc2) = weights
    nb, tok_rows, tok_cols, chan = tokens.shape
    dim = w_reduce.shape[1]
    ff = w_fc1.shape[1]
    n_heads = rel_table.shape[1]
    head_dim = dim // n_heads
    seq = rel_index.shape[0]
    window = math.isqrt(seq)
    n = 2 * seq
    groups = n_heads // HEAD_GROUP
    lanes = HEAD_GROUP * seq
    table_pad = -(-rel_table.shape[0] // 128) * 128
    perm4, perm_w = merge_perm(window, tok_cols), window_perm(window)
    table_t = jnp.pad(rel_table.astype(F32).T, ((0, 0), (0, table_pad - rel_table.shape[0])))

    pos = call(pos_kernel, (1,), (table_t, rel_index), [whole(table_t.shape), whole(rel_index.shape)],
               [sds((groups, seq, lanes), F32)], [out_whole((groups, seq, lanes))], [], 10**7, "pos")[0]

    ins = (tokens, perm4, pos, norm_merge, w_reduce, norm_attn, w_qkv, b_qkv, w_proj, b_proj)
    outs = [sds((nb, n, 4 * chan), BF), sds((nb, n, dim), BF), sds((nb, n, 3 * dim), BF), sds((nb, n, dim), BF),
            sds((nb, 2, groups, 1, lanes), F32), sds((nb, n, dim), BF)]
    raw, h0, qkv, att, lse, h1 = call(
        functools.partial(fwd_kernel, head_dim=head_dim, seq=seq), (nb,), ins,
        [band(tokens.shape)] + [whole(a.shape) for a in ins[1:]], outs, [band(o.shape) for o in outs], [], 8 * 10**9, "fwd")

    ins = (h1, cot.reshape(nb, n, dim), perm_w, norm_mlp, w_fc1, b_fc1, w_fc2, b_fc2)
    tok = lambda width, dtype=BF: sds((nb, n, width), dtype)
    outs = [tok(dim), tok(dim, F32), tok(ff), tok(ff), tok(dim), tok(dim), sds((1, ff), F32), sds((1, dim), F32), sds((2, dim), F32)]
    result, dh1, hid, dpre, b_in, cot_w, g_b1, g_b2, g_nb = call(
        mlp_kernel, (nb,), ins, [band(ins[0].shape), band(ins[1].shape)] + [whole(a.shape) for a in ins[2:]],
        outs, [band(o.shape) for o in outs[:6]] + [out_whole(o.shape) for o in outs[6:]], [], 12 * 10**9, "mlp")

    ins = (dh1, raw, h0, qkv, lse, perm4, pos, norm_merge, w_reduce, norm_attn, w_qkv, w_proj)
    outs = [sds(tokens.shape, BF), tok(dim), tok(dim), tok(3 * dim), tok(4 * chan), tok(dim), sds((1, dim), F32),
            sds((1, 3 * dim), F32), sds((2, dim), F32), sds((2, 4 * chan), F32), sds((groups, seq, lanes), F32)]
    g_tok, dh1_bf, a_in, dqkv, m_in, dh0, g_bp, g_bq, g_na, g_nm, g_pos = call(
        functools.partial(bwd_kernel, head_dim=head_dim, seq=seq), (nb,), ins,
        [band(a.shape) for a in ins[:5]] + [whole(a.shape) for a in ins[5:]],
        outs, [band(o.shape) for o in outs[:6]] + [out_whole(o.shape) for o in outs[6:]],
        [pltpu.VMEM((n, dim), BF), pltpu.VMEM((n, 3 * dim), F32)], 12 * 10**9, "bwd")

    pairs = [(hid, cot_w), (b_in, dpre), (m_in, dh0), (a_in, dqkv), (att, dh1_bf)]
    return result, g_tok, [tuple(x.reshape(nb * n, -1) for x in pair) for pair in pairs], [g_nm, g_na, g_nb, g_bq, g_bp, g_b1, g_b2], g_pos


ORDERS = (('core', 'x', 'y', 'z0', 'z1'), ('core', 'y', 'x', 'z0', 'z1'), ('core', 'z0', 'z1', 'x', 'y'), ('core', 'z0', 'z1', 'y', 'x'))
HALVES = (128, 64, 32, 16, 8)
LAND = (0, 128, 192, 224, 240)
WIDTH = 512
STARTS = tuple(range(1, 23, 2))
Z_FIRST = 5
TABLE_STEP = 8


def place():
    dp, sp = lax.axis_index('dp'), lax.axis_index('sp')
    bits = {'core': sp % 2, 'x': sp // 2, 'y': dp % 2, 'z0': (dp // 2) % 2, 'z1': dp // 4}
    unit = {'core': (0, 1), 'x': (0, 2), 'y': (1, 0), 'z0': (2, 0), 'z1': (4, 0)}
    peers = {k: (dp + (1 - 2 * b) * unit[k][0], sp + (1 - 2 * b) * unit[k][1]) for k, b in bits.items()}
    return bits, peers


class Stream:
    def __init__(self, order, other, swap, buf, land, send, recv):
        bits, peers = place()
        pick = lambda a, b: a if a is b else jnp.where(swap, b, a)
        self.buf, self.land, self.send, self.recv = buf, land, send, recv
        self.bits = [pick(bits[a], bits[b]) for a, b in zip(order, other)]
        self.peers = [tuple(pick(p, q) for p, q in zip(peers[a], peers[b])) for a, b in zip(order, other)]
        offs = [0]
        for b, half in zip(self.bits, HALVES):
            offs.append(offs[-1] + b * half)
        self.offs = offs

    def rows(self, start, size):
        return pl.ds(pl.multiple_of(start, 8), size)

    def copy(self, k):
        j = k if k < 5 else 9 - k
        half = HALVES[j]
        if k == 0:
            src = self.buf.at[self.rows((1 - self.bits[0]) * half, half)]
        elif k < 5:
            src = self.land.at[self.rows(LAND[j - 1] + (1 - self.bits[j]) * half, half)]
        else:
            src = self.buf.at[self.rows(self.offs[j + 1], half)]
        dst = self.land.at[pl.ds(LAND[j], half)] if k < 5 else self.buf.at[self.rows(self.offs[j + 1], half)]
        return pltpu.make_async_remote_copy(src_ref=src, dst_ref=dst, send_sem=self.send.at[k], recv_sem=self.recv.at[k],
                                            device_id=self.peers[j], device_id_type=pl.DeviceIdType.MESH)

    def finish(self, k):
        self.copy(k).wait()
        if k < 5:
            half = HALVES[k]
            if k == 0:
                kept = self.buf[self.rows(self.bits[0] * half, half), :]
            else:
                kept = self.land[self.rows(LAND[k - 1] + self.bits[k] * half, half), :]
            total = self.land[pl.ds(LAND[k], half), :] + kept
            if k < 4:
                self.land[pl.ds(LAND[k], half), :] = total
            else:
                self.buf[self.rows(self.offs[5], half), :] = total

    def advance(self, k):
        if k > 0:
            self.finish(k - 1)
        if k < 10:
            self.copy(k).start()


def add_table(pos_s, idx_ref, table_s, first):
    row = lax.broadcasted_iota(jnp.int32, (table_s.shape[1], idx_ref.shape[1]), 0)
    acc = table_s[...]
    for j in range(TABLE_STEP):
        m = first + j
        hot = jnp.where(row == idx_ref[pl.ds(m, 1), :], 1.0, 0.0).astype(BF)
        val = pos_s[m]
        hi = val.astype(BF)
        rest = val - hi.astype(F32)
        mid = rest.astype(BF)
        low = (rest - mid.astype(F32)).astype(BF)
        acc = acc + dot_nt(jnp.concatenate([hi, mid, low], axis=0), hot)
    table_s[...] = acc


def reduce_kernel(*refs, n, n_small):
    refs = list(refs)
    take = lambda count: [refs.pop(0) for _ in range(count)]
    pairs, smalls, (gpos_ref, idx_ref, res_in) = take(2 * n), take(n_small), take(3)
    outs, (small_out, res_out), held = take(n), take(2), take(2 * n)
    buf, land, small_land, pos_s, table_s, idx_s, send, recv, small_send, small_recv, sem_in, sem_out, res_send, res_recv, res_here = refs
    seq = idx_ref.shape[0]
    n_heads = pos_s.shape[1]
    total = buf.shape[0]
    loads = [pltpu.make_async_copy(a, b, sem_in.at[i]) for i, (a, b) in enumerate(zip(pairs, held))]
    for load in loads:
        load.start()
    groups, base = [], 0
    for i, out in enumerate(outs):
        count = out.shape[0] * out.shape[1] // (512 * WIDTH)
        groups.append((base, count, held[2 * i], held[2 * i + 1], out, loads[2 * i:2 * i + 2]))
        base += count

    def block(out, j, side):
        wide = out.shape[1] // WIDTH
        row0, col0 = j // wide * 512 + side * 256, j % wide * WIDTH
        return out.at[pl.ds(pl.multiple_of(row0, 256), 256), pl.ds(pl.multiple_of(col0, WIDTH), WIDTH)]

    def part(ref, j):
        return ref[...] if ref.shape[1] == WIDTH else ref[:, pl.ds(pl.multiple_of(j * WIDTH, WIDTH), WIDTH)]

    peers = place()[1]
    dp, sp = lax.axis_index('dp'), lax.axis_index('sp')
    ring = res_in.shape[0]
    barrier = pltpu.get_barrier_semaphore()
    for peer in [peers[k] for k in ORDERS[0]] + [(dp, 3 - sp)]:
        pl.semaphore_signal(barrier, inc=1, device_id=peer, device_id_type=pl.DeviceIdType.MESH)
    pl.semaphore_wait(barrier, 6)
    moves = [pltpu.make_async_copy(res_in.at[sp], res_out.at[sp], res_here.at[0])]
    for d in range(1, ring):
        to = lax.rem(sp + d, ring)
        moves.append(pltpu.make_async_remote_copy(src_ref=res_in.at[to], dst_ref=res_out.at[sp], send_sem=res_send.at[d], recv_sem=res_recv.at[d],
                                                  device_id=(dp, to), device_id_type=pl.DeviceIdType.MESH))
    for move in moves:
        move.start()
    table_s[...] = jnp.zeros(table_s.shape, F32)
    room = small_out.shape[0] - table_s.shape[0] * table_s.shape[1] // (3 * 128)
    small_out[0:room, :] = jnp.zeros((room, 128), F32)
    for ref, r, c, at in small_rows([x.shape for x in smalls]):
        small_out[at:at + 1, :] = smalls[ref][r:r + 1, c:c + 128]
    table_ticks = seq // TABLE_STEP
    small_at = table_ticks + 2
    slots = total // 2

    def tick(t, carry):
        for k in range(10, -1, -1):
            u = t - STARTS[k]

            @pl.when((u >= 0) & (u < slots))
            def _():
                swap = lax.rem(u, Z_FIRST) == Z_FIRST - 1
                for side in range(2):
                    s = 2 * u + side
                    Stream(ORDERS[side], ORDERS[2 + side], swap, buf.at[s], land.at[s], send.at[s], recv.at[s]).advance(k)
                if k == 10:
                    for first, count, left, right, out, loads in groups:
                        @pl.when((u >= first) & (u < first + count))
                        def _():
                            for side in range(2):
                                s = 2 * u + side
                                pltpu.make_async_copy(buf.at[s], block(out, u - first, side), sem_out.at[s]).start()

            @pl.when(t == small_at + k)
            def _():
                Stream(ORDERS[0], ORDERS[0], None, small_out, small_land, small_send, small_recv).advance(k)

        for first, count, left, right, out, loads in groups:
            @pl.when(t == first)
            def _():
                for load in loads:
                    load.wait()

            @pl.when((t >= first) & (t < first + count))
            def _():
                value = dot_tn(part(left, t - first), part(right, t - first))
                buf[2 * t] = value[:256]
                buf[2 * t + 1] = value[256:]

        @pl.when(t == 0)
        def _():
            idx_s[...] = idx_ref[...].T
            for g in range(gpos_ref.shape[0]):
                for h in range(HEAD_GROUP):
                    pos_s[:, g * HEAD_GROUP + h, :] = gpos_ref[g, :, h * seq:(h + 1) * seq]

        @pl.when((t >= 1) & (t < 1 + table_ticks))
        def _():
            add_table(pos_s, idx_s, table_s, (t - 1) * TABLE_STEP)

        @pl.when(t == 1 + table_ticks)
        def _():
            summed = table_s[0:n_heads] + table_s[n_heads:2 * n_heads] + table_s[2 * n_heads:3 * n_heads]
            for p in range(table_s.shape[1] // 128):
                small_out[room + p * n_heads:room + (p + 1) * n_heads, :] = summed[:, p * 128:(p + 1) * 128]
        return carry
    lax.fori_loop(0, max(slots + STARTS[10] + 1, small_at + 11), tick, 0)

    def drain(s, carry):
        pltpu.make_async_copy(buf.at[s], block(outs[0], 0, 0), sem_out.at[s]).wait()
        return carry
    lax.fori_loop(0, total, drain, 0)
    for move in moves:
        move.wait()


def small_rows(shapes):
    rows = []
    for ref, shape in enumerate(shapes):
        for r in range(shape[0]):
            for c in range(0, shape[1], 128):
                rows.append((ref, r, c, len(rows)))
    return rows


def reduce_all(pairs, smalls, g_pos, rel_index, result, n_heads, table_len):
    shapes = [(a.shape[1], b.shape[1]) for a, b in pairs]
    total = sum(a * b // (256 * WIDTH) for a, b in shapes)
    n = len(pairs)
    flat = [x for pair in pairs for x in pair]
    seq = rel_index.shape[0]
    table_pad = -(-table_len // 128) * 128
    vmem, hbm = pl.BlockSpec(memory_space=pltpu.VMEM), pl.BlockSpec(memory_space=pl.ANY)
    outs = [sds(shape, F32) for shape in shapes] + [sds((256, 128), F32), sds(result.shape, result.dtype)]
    dma = pltpu.SemaphoreType.DMA
    ring = result.shape[0]
    return pl.pallas_call(
        functools.partial(reduce_kernel, n=n, n_small=len(smalls)),
        in_specs=[hbm] * (2 * n) + [vmem] * (len(smalls) + 2) + [hbm], out_specs=[hbm] * n + [vmem, hbm], out_shape=outs,
        scratch_shapes=[pltpu.VMEM(x.shape, x.dtype) for x in flat] + [
            pltpu.VMEM((total, 256, WIDTH), F32), pltpu.VMEM((total, 248, WIDTH), F32), pltpu.VMEM((248, 128), F32), pltpu.VMEM((seq, n_heads, seq), F32),
            pltpu.VMEM((3 * n_heads, table_pad), F32), pltpu.VMEM((seq, seq), jnp.int32), dma((total, 10)), dma((total, 10)), dma((10,)), dma((10,)),
            dma((2 * n,)), dma((total,)), dma((ring,)), dma((ring,)), dma((1,))],
        name="reduce", compiler_params=pltpu.CompilerParams(collective_id=0, has_side_effects=True, vmem_limit_bytes=63 * 1024 * 1024))(
            *flat, *smalls, g_pos, rel_index, result)


def finish_kernel(*refs, n, cuts):
    refs = list(refs)
    take = lambda count: [refs.pop(0) for _ in range(count)]
    ins, (small,), outs, smalls, (table,), bufs, (sem_in, sem_out) = take(n), take(1), take(n), take(len(refs) - n - 3), take(1), take(n), refs
    stores = []
    loads = []
    for i, (a, b, c) in enumerate(zip(ins, bufs, outs)):
        step = a.shape[0] // cuts
        for p in range(cuts):
            at = pl.ds(p * step, step)
            loads.append(pltpu.make_async_copy(a.at[at], b.at[at], sem_in.at[i, p]))
            stores.append(pltpu.make_async_copy(b.at[at], c.at[at], sem_out.at[i, p]))
    for load in loads:
        load.start()
    for ref, r, c, at in small_rows([x.shape for x in smalls]):
        smalls[ref][r:r + 1, c:c + 128] = small[at:at + 1, :]
    n_heads, table_len = table.shape
    pieces = -(-table_len // 128)
    first = small.shape[0] - pieces * n_heads
    full = jnp.concatenate([small[first + p * n_heads:first + (p + 1) * n_heads, :] for p in range(pieces)], axis=1)
    table[...] = full[:, :table_len]
    for load, store in zip(loads, stores):
        load.wait()
        store.start()
    for store in stores:
        store.wait()


def finish(large, small, small_shapes, n_heads, table_len):
    n, cuts = len(large), 4
    vmem, hbm = pl.BlockSpec(memory_space=pltpu.VMEM), pl.BlockSpec(memory_space=pl.ANY)
    outs = [sds(x.shape, x.dtype) for x in large] + [sds(shape, F32) for shape in small_shapes] + [sds((n_heads, table_len), F32)]
    got = pl.pallas_call(
        functools.partial(finish_kernel, n=n, cuts=cuts), in_specs=[hbm] * n + [vmem], out_specs=[hbm] * n + [vmem] * (len(outs) - n), out_shape=outs,
        scratch_shapes=[pltpu.VMEM(x.shape, x.dtype) for x in large] + [pltpu.SemaphoreType.DMA((n, cuts)), pltpu.SemaphoreType.DMA((n, cuts))],
        name="finish", compiler_params=pltpu.CompilerParams(vmem_limit_bytes=VMEM_LIMIT))(*large, small)
    return got[:n], got[n:-1], got[-1].T


def solution(mesh):
    def device_fn(tokens, grad_out, rel_index, *weights):
        cot = lax.all_to_all(grad_out, 'sp', 1, 0, tiled=True)
        result, g_tok, pairs, smalls, g_pos = local_step(tokens, cot, rel_index, weights)
        table_len, n_heads = weights[5].shape
        *grads, small, result = reduce_all(pairs, smalls, g_pos, rel_index, result, n_heads, table_len)
        large, smalls, g_table = finish(grads + [result], small, [x.shape for x in smalls], n_heads, table_len)
        g_w2, g_w1, g_wr, g_wq, g_wp, result = large
        g_nm, g_na, g_nb, g_bq, g_bp, g_b1, g_b2 = smalls
        return (result.reshape(grad_out.shape), g_tok, g_nm, g_wr, g_na, g_wq, g_bq.reshape(-1), g_table, g_wp, g_bp.reshape(-1), g_nb,
                g_w1, g_b1.reshape(-1), g_w2, g_b2.reshape(-1))

    rep_specs = (P(),) * 13
    return jax.shard_map(device_fn, mesh=mesh, in_specs=(P('dp', 'sp'), P(('dp', 'sp')), P()) + rep_specs, out_specs=(P(('dp', 'sp')), P('dp', 'sp')) + rep_specs, check_vma=False)
```

```python
import functools
import math
import numpy as np
import jax
import jax.numpy as jnp
from jax import lax
from jax.experimental import pallas as pl
from jax.experimental.pallas import tpu as pltpu
from jax.sharding import PartitionSpec as P

NORM_EPS = 1e-5
BF, F32 = jnp.bfloat16, jnp.float32
VMEM_LIMIT = 60 * 1024 * 1024
HEAD_GROUP = 8
GROUP_ROWS = 4


def dot_nn(a, b):
    return lax.dot_general(a, b, (((1,), (0,)), ((), ())), preferred_element_type=F32)


def dot_nt(a, b):
    return lax.dot_general(a, b, (((1,), (1,)), ((), ())), preferred_element_type=F32)


def dot_tn(a, b):
    return lax.dot_general(a, b, (((0,), (0,)), ((), ())), preferred_element_type=F32)


def norm_hat(x):
    mu = jnp.mean(x, axis=-1, keepdims=True)
    xc = x - mu
    rstd = lax.rsqrt(jnp.mean(xc * xc, axis=-1, keepdims=True) + NORM_EPS)
    return xc * rstd, rstd


def norm_fwd(x, norm_ref):
    hat, rstd = norm_hat(x)
    return hat * norm_ref[0:1, :].astype(F32) + norm_ref[1:2, :].astype(F32), hat, rstd


def norm_bwd(dy, hat, rstd, norm_ref):
    dhat = dy * norm_ref[0:1, :].astype(F32)
    m1 = jnp.mean(dhat, axis=-1, keepdims=True)
    m2 = jnp.mean(dhat * hat, axis=-1, keepdims=True)
    dx = rstd * (dhat - m1 - hat * m2)
    return dx, jnp.sum(dy * hat, axis=0, keepdims=True), jnp.sum(dy, axis=0, keepdims=True)


def head_masks(width, head_dim, dtype):
    lane = lax.broadcasted_iota(jnp.int32, (1, width), 1) // head_dim
    return [jnp.where(lane == h, 1.0, 0.0).astype(dtype) for h in range(width // head_dim)]


def stack_heads(x, masks):
    return jnp.concatenate([x * m for m in masks], axis=0)


def unstack_heads(x, masks, seq):
    total = x[0:seq] * masks[0]
    for h in range(1, len(masks)):
        total = total + x[h * seq:(h + 1) * seq] * masks[h]
    return total


def pos_kernel(table_ref, idx_ref, pos_ref):
    seq = idx_ref.shape[0]
    n_pieces = table_ref.shape[1] // 128
    for g in range(pos_ref.shape[0]):
        wide = jnp.concatenate([idx_ref[...].T] * HEAD_GROUP, axis=1)
        for c in range(wide.shape[1] // 128):
            idx = wide[:, c * 128:(c + 1) * 128]
            low, high = idx & 127, idx >> 7
            lane = lax.broadcasted_iota(jnp.int32, idx.shape, 1) + c * 128
            out = jnp.zeros(idx.shape, F32)
            for h in range((c * 128) // seq, (c * 128 + 127) // seq + 1):
                val = jnp.zeros(idx.shape, F32)
                for t in range(n_pieces):
                    row = table_ref[g * HEAD_GROUP + h:g * HEAD_GROUP + h + 1, t * 128:(t + 1) * 128]
                    got = jnp.take_along_axis(jnp.broadcast_to(row, idx.shape), low, axis=1)
                    val = jnp.where(high == t, got, val)
                out = jnp.where((lane >= h * seq) & (lane < (h + 1) * seq), val, out)
            pos_ref[g, :, c * 128:(c + 1) * 128] = out


def fwd_kernel(tok_ref, perm_ref, pos_ref, nm_ref, wr_ref, na_ref, wq_ref, bq_ref, wp_ref, bp_ref,
               raw_ref, h0_ref, qkv_ref, att_ref, lse_ref, h1_ref, *, head_dim, seq):
    dim = h0_ref.shape[2]
    x = tok_ref[0].reshape(-1, tok_ref.shape[3])
    step = perm_ref.shape[0]
    quad = step // 4
    piece = quad // 2
    for g in range(x.shape[0] // step):
        y = dot_nn(perm_ref[...], x[g * step:(g + 1) * step])
        for w in range(2):
            cat = jnp.concatenate([y[p * quad + w * piece:p * quad + (w + 1) * piece] for p in range(4)], axis=1)
            raw_ref[0, w * seq + g * piece:w * seq + (g + 1) * piece, :] = cat.astype(BF)
    merged = norm_fwd(raw_ref[0].astype(F32), nm_ref)[0].astype(BF)
    h0 = dot_nn(merged, wr_ref[...]).astype(BF)
    h0_ref[0] = h0
    a = norm_fwd(h0.astype(F32), na_ref)[0].astype(BF)
    qkv_ref[0] = (dot_nn(a, wq_ref[...]) + bq_ref[...].astype(F32).reshape(1, -1)).astype(BF)
    width = HEAD_GROUP * head_dim
    masks, masks_f = head_masks(width, head_dim, BF), head_masks(width, head_dim, F32)
    scale = head_dim ** -0.5
    for w in range(2):
        rows = slice(w * seq, (w + 1) * seq)
        for g in range(dim // width):
            cols = [slice(t * dim + g * width, t * dim + (g + 1) * width) for t in range(3)]
            q, k, v = (qkv_ref[0, rows, c] for c in cols)
            s = dot_nt(k, stack_heads(q, masks)) * scale + pos_ref[g]
            top = jnp.max(s, axis=0, keepdims=True)
            e = jnp.exp(s - top)
            den = jnp.sum(e, axis=0, keepdims=True)
            prob = (e * (1.0 / den)).astype(BF)
            lse_ref[0, w, g] = top + jnp.log(den)
            att_ref[0, rows, g * width:(g + 1) * width] = unstack_heads(dot_tn(prob, v), masks_f, seq).astype(BF)
    h1 = h0_ref[0].astype(F32) + dot_nn(att_ref[0], wp_ref[...]) + bp_ref[...].astype(F32).reshape(1, -1)
    h1_ref[0] = h1.astype(BF)


def mlp_kernel(h1_ref, cot_ref, perm_ref, nb_ref, w1_ref, b1_ref, w2_ref, b2_ref,
               out_ref, dh1_ref, hid_ref, dpre_ref, b_ref, cotw_ref, gb1_ref, gb2_ref, gnb_ref):
    i = pl.program_id(0)

    @pl.when(i == 0)
    def _():
        gb1_ref[...] = jnp.zeros(gb1_ref.shape, F32)
        gb2_ref[...] = jnp.zeros(gb2_ref.shape, F32)
        gnb_ref[...] = jnp.zeros(gnb_ref.shape, F32)

    h1 = h1_ref[0].astype(F32)
    normed, hat, rstd = norm_fwd(h1, nb_ref)
    nb = normed.astype(BF)
    b_ref[0] = nb
    cot = dot_nn(perm_ref[...], cot_ref[0])
    cot_bf = cot.astype(BF)
    cotw_ref[0] = cot_bf
    gb2_ref[...] += jnp.sum(cot, axis=0, keepdims=True)
    out = h1 + b2_ref[...].astype(F32).reshape(1, -1)
    d_norm = jnp.zeros(h1.shape, F32)
    chunk = 512
    for c in range(w1_ref.shape[1] // chunk):
        cols = slice(c * chunk, (c + 1) * chunk)
        pre = dot_nn(nb, w1_ref[:, cols]) + b1_ref[cols].astype(F32).reshape(1, -1)
        phi = 0.5 + 0.5 * lax.erf(pre * math.sqrt(0.5))
        hid = (pre * phi).astype(BF)
        hid_ref[0, :, cols] = hid
        out = out + dot_nn(hid, w2_ref[cols, :])
        d_act = phi + pre * (jnp.exp(pre * pre * -0.5) * (1.0 / math.sqrt(2.0 * math.pi)))
        d_pre = dot_nt(cot_bf, w2_ref[cols, :]) * d_act
        gb1_ref[:, cols] += jnp.sum(d_pre, axis=0, keepdims=True)
        d_pre_bf = d_pre.astype(BF)
        dpre_ref[0, :, cols] = d_pre_bf
        d_norm = d_norm + dot_nt(d_pre_bf, w1_ref[:, cols])
    out_ref[0] = dot_tn(perm_ref[...], out.astype(BF)).astype(BF)
    dx, g_gain, g_shift = norm_bwd(d_norm, hat, rstd, nb_ref)
    gnb_ref[0:1, :] += g_gain
    gnb_ref[1:2, :] += g_shift
    dh1_ref[0] = cot + dx


def bwd_kernel(dh1_ref, h0_ref, qkv_ref, lse_ref, pos_ref, na_ref, wq_ref, wp_ref,
               dh1b_ref, a_ref, dqkv_ref, dh0_ref, gbp_ref, gbq_ref, gna_ref, gpos_ref,
               datt_s, dqkv_f, *, head_dim, seq):
    i = pl.program_id(0)
    dim = h0_ref.shape[2]

    @pl.when(i == 0)
    def _():
        for ref in (gbp_ref, gbq_ref, gna_ref, gpos_ref):
            ref[...] = jnp.zeros(ref.shape, F32)

    dh1 = dh1_ref[0]
    gbp_ref[...] += jnp.sum(dh1, axis=0, keepdims=True)
    dh1_bf = dh1.astype(BF)
    dh1b_ref[0] = dh1_bf
    datt_s[...] = dot_nt(dh1_bf, wp_ref[...]).astype(BF)
    width = HEAD_GROUP * head_dim
    masks, masks_f = head_masks(width, head_dim, BF), head_masks(width, head_dim, F32)
    scale = head_dim ** -0.5
    for w in range(2):
        rows = slice(w * seq, (w + 1) * seq)
        for g in range(dim // width):
            cols = [slice(t * dim + g * width, t * dim + (g + 1) * width) for t in range(3)]
            q, k, v = (qkv_ref[0, rows, c] for c in cols)
            qm = stack_heads(q, masks)
            dam = stack_heads(datt_s[rows, g * width:(g + 1) * width], masks)
            prob = jnp.exp(dot_nt(k, qm) * scale + pos_ref[g] - lse_ref[0, w, g])
            d_prob = dot_nt(v, dam)
            dqkv_f[rows, cols[2]] = dot_nn(prob.astype(BF), dam)
            delta = jnp.sum(d_prob * prob, axis=0, keepdims=True)
            ds = prob * (d_prob - delta)
            gpos_ref[g] += ds
            ds_bf = (ds * scale).astype(BF)
            dqkv_f[rows, cols[1]] = dot_nn(ds_bf, qm)
            dqkv_f[rows, cols[0]] = unstack_heads(dot_tn(ds_bf, k), masks_f, seq)
    gbq_ref[...] += jnp.sum(dqkv_f[...], axis=0, keepdims=True)
    dqkv_bf = dqkv_f[...].astype(BF)
    dqkv_ref[0] = dqkv_bf
    d_a = dot_nt(dqkv_bf, wq_ref[...])
    normed, hat, rstd = norm_fwd(h0_ref[0].astype(F32), na_ref)
    a_ref[0] = normed.astype(BF)
    dx, g_gain, g_shift = norm_bwd(d_a, hat, rstd, na_ref)
    gna_ref[0:1, :] += g_gain
    gna_ref[1:2, :] += g_shift
    dh0_bf = (dh1 + dx).astype(BF)
    dh0_ref[0] = dh0_bf


def merge_backward(rows, raw_ref, dh0_ref, perm_ref, nm_ref, wr_ref, gnm_s, stage):
    d_m = dot_nt(dh0_ref[rows, :], wr_ref[...])
    normed, hat, rstd = norm_fwd(raw_ref[rows, :].astype(F32), nm_ref)
    raw_ref[rows, :] = normed.astype(BF)
    dx, g_gain, g_shift = norm_bwd(d_m, hat, rstd, nm_ref)
    gnm_s[0:1, :] += g_gain
    gnm_s[1:2, :] += g_shift
    d_raw = dx.astype(BF)
    step = perm_ref.shape[0]
    piece = step // 8
    seq = d_raw.shape[0] // 2
    chan = d_raw.shape[1] // 4
    tok_rows = step // stage.shape[1]
    for g in range(seq // piece):
        y = jnp.concatenate([d_raw[w * seq + g * piece:w * seq + (g + 1) * piece, p * chan:(p + 1) * chan]
                             for p in range(4) for w in range(2)], axis=0)
        stage[g * tok_rows:(g + 1) * tok_rows] = dot_tn(perm_ref[...], y).astype(BF).reshape(tok_rows, stage.shape[1], chan)


def whole(shape):
    zeros = (0,) * len(shape)
    return pl.BlockSpec(shape, lambda i: zeros, pipeline_mode=pl.Buffered(1))


def out_whole(shape):
    zeros = (0,) * len(shape)
    return pl.BlockSpec(shape, lambda i: zeros)


def band(shape):
    zeros = (0,) * (len(shape) - 1)
    return pl.BlockSpec((1,) + shape[1:], lambda i: (i,) + zeros)


def sds(shape, dtype):
    return jax.ShapeDtypeStruct(shape, dtype)


def call(kernel, grid, ins, in_specs, outs, out_specs, scratch, flops, name):
    moved = sum(math.prod(a.shape) * a.dtype.itemsize for a in list(ins) + list(outs))
    return pl.pallas_call(
        kernel, grid=grid, in_specs=in_specs, out_specs=out_specs, out_shape=outs, scratch_shapes=scratch, name=name,
        cost_estimate=pl.CostEstimate(flops=flops, bytes_accessed=moved, transcendentals=0),
        compiler_params=pltpu.CompilerParams(vmem_limit_bytes=VMEM_LIMIT, dimension_semantics=("arbitrary",) * len(grid)))(*ins)


def merge_perm(window, cols):
    rows_in = 2 * GROUP_ROWS * cols
    perm = np.zeros((rows_in, rows_in), np.float32)
    out = 0
    for quad in range(4):
        c, r = quad // 2, quad % 2
        for w in range(2):
            for i in range(GROUP_ROWS):
                for j in range(window):
                    perm[out, (2 * i + r) * cols + 2 * (w * window + j) + c] = 1.0
                    out += 1
    return jnp.asarray(perm, BF)


def window_perm(window):
    n = 2 * window * window
    perm = np.zeros((n, n), np.float32)
    for w in range(2):
        for i in range(window):
            for j in range(window):
                perm[(w * window + i) * window + j, (i * 2 + w) * window + j] = 1.0
    return jnp.asarray(perm, BF)


def local_step(tokens, cot, rel_index, weights):
    (norm_merge, w_reduce, norm_attn, w_qkv, b_qkv, rel_table, w_proj, b_proj, norm_mlp, w_fc1, b_fc1, w_fc2, b_fc2) = weights
    nb, tok_rows, tok_cols, chan = tokens.shape
    dim = w_reduce.shape[1]
    ff = w_fc1.shape[1]
    n_heads = rel_table.shape[1]
    head_dim = dim // n_heads
    seq = rel_index.shape[0]
    window = math.isqrt(seq)
    n = 2 * seq
    groups = n_heads // HEAD_GROUP
    lanes = HEAD_GROUP * seq
    table_pad = -(-rel_table.shape[0] // 128) * 128
    perm4, perm_w = merge_perm(window, tok_cols), window_perm(window)
    table_t = jnp.pad(rel_table.astype(F32).T, ((0, 0), (0, table_pad - rel_table.shape[0])))

    pos = call(pos_kernel, (1,), (table_t, rel_index), [whole(table_t.shape), whole(rel_index.shape)],
               [sds((groups, seq, lanes), F32)], [out_whole((groups, seq, lanes))], [], 10**7, "pos")[0]

    ins = (tokens, perm4, pos, norm_merge, w_reduce, norm_attn, w_qkv, b_qkv, w_proj, b_proj)
    outs = [sds((nb, n, 4 * chan), BF), sds((nb, n, dim), BF), sds((nb, n, 3 * dim), BF), sds((nb, n, dim), BF),
            sds((nb, 2, groups, 1, lanes), F32), sds((nb, n, dim), BF)]
    raw, h0, qkv, att, lse, h1 = call(
        functools.partial(fwd_kernel, head_dim=head_dim, seq=seq), (nb,), ins,
        [band(tokens.shape)] + [whole(a.shape) for a in ins[1:]], outs, [band(o.shape) for o in outs], [], 8 * 10**9, "fwd")

    ins = (h1, cot.reshape(nb, n, dim), perm_w, norm_mlp, w_fc1, b_fc1, w_fc2, b_fc2)
    tok = lambda width, dtype=BF: sds((nb, n, width), dtype)
    outs = [tok(dim), tok(dim, F32), tok(ff), tok(ff), tok(dim), tok(dim), sds((1, ff), F32), sds((1, dim), F32), sds((2, dim), F32)]
    result, dh1, hid, dpre, b_in, cot_w, g_b1, g_b2, g_nb = call(
        mlp_kernel, (nb,), ins, [band(ins[0].shape), band(ins[1].shape)] + [whole(a.shape) for a in ins[2:]],
        outs, [band(o.shape) for o in outs[:6]] + [out_whole(o.shape) for o in outs[6:]], [], 12 * 10**9, "mlp")

    ins = (dh1, h0, qkv, lse, pos, norm_attn, w_qkv, w_proj)
    outs = [tok(dim), tok(dim), tok(3 * dim), tok(dim), sds((1, dim), F32), sds((1, 3 * dim), F32), sds((2, dim), F32), sds((groups, seq, lanes), F32)]
    dh1_bf, a_in, dqkv, dh0, g_bp, g_bq, g_na, g_pos = call(
        functools.partial(bwd_kernel, head_dim=head_dim, seq=seq), (nb,), ins,
        [band(a.shape) for a in ins[:4]] + [whole(a.shape) for a in ins[4:]],
        outs, [band(o.shape) for o in outs[:4]] + [out_whole(o.shape) for o in outs[4:]],
        [pltpu.VMEM((n, dim), BF), pltpu.VMEM((n, 3 * dim), F32)], 12 * 10**9, "bwd")

    pairs = [(hid, cot_w), (b_in, dpre), (a_in, dqkv), (att, dh1_bf), (raw, dh0)]
    return (result, [tuple(x.reshape(nb * n, -1) for x in pair) for pair in pairs], [g_na, g_nb, g_bq, g_bp, g_b1, g_b2],
            [perm4, norm_merge, w_reduce, g_pos, rel_index])


ORDERS = (('core', 'x', 'y', 'z0', 'z1'), ('core', 'y', 'x', 'z0', 'z1'), ('core', 'z0', 'z1', 'x', 'y'), ('core', 'z0', 'z1', 'y', 'x'))
HALVES = (128, 64, 32, 16, 8)
LAND = (0, 128, 192, 224, 240)
WIDTH = 512
STARTS = tuple(range(1, 23, 2))
Z_FIRST = 5
TABLE_STEP = 12
TABLE_FROM = 9


def place():
    dp, sp = lax.axis_index('dp'), lax.axis_index('sp')
    bits = {'core': sp % 2, 'x': sp // 2, 'y': dp % 2, 'z0': (dp // 2) % 2, 'z1': dp // 4}
    unit = {'core': (0, 1), 'x': (0, 2), 'y': (1, 0), 'z0': (2, 0), 'z1': (4, 0)}
    peers = {k: (dp + (1 - 2 * b) * unit[k][0], sp + (1 - 2 * b) * unit[k][1]) for k, b in bits.items()}
    return bits, peers


class Stream:
    def __init__(self, order, other, swap, buf, land, send, recv):
        bits, peers = place()
        pick = lambda a, b: a if a is b else jnp.where(swap, b, a)
        self.buf, self.land, self.send, self.recv = buf, land, send, recv
        self.bits = [pick(bits[a], bits[b]) for a, b in zip(order, other)]
        self.peers = [tuple(pick(p, q) for p, q in zip(peers[a], peers[b])) for a, b in zip(order, other)]
        offs = [0]
        for b, half in zip(self.bits, HALVES):
            offs.append(offs[-1] + b * half)
        self.offs = offs

    def rows(self, start, size):
        return pl.ds(pl.multiple_of(start, 8), size)

    def copy(self, k):
        j = k if k < 5 else 9 - k
        half = HALVES[j]
        if k == 0:
            src = self.buf.at[self.rows((1 - self.bits[0]) * half, half)]
        elif k < 5:
            src = self.land.at[self.rows(LAND[j - 1] + (1 - self.bits[j]) * half, half)]
        else:
            src = self.buf.at[self.rows(self.offs[j + 1], half)]
        dst = self.land.at[pl.ds(LAND[j], half)] if k < 5 else self.buf.at[self.rows(self.offs[j + 1], half)]
        return pltpu.make_async_remote_copy(src_ref=src, dst_ref=dst, send_sem=self.send.at[k], recv_sem=self.recv.at[k],
                                            device_id=self.peers[j], device_id_type=pl.DeviceIdType.MESH)

    def finish(self, k):
        self.copy(k).wait()
        if k < 5:
            half = HALVES[k]
            if k == 0:
                kept = self.buf[self.rows(self.bits[0] * half, half), :]
            else:
                kept = self.land[self.rows(LAND[k - 1] + self.bits[k] * half, half), :]
            total = self.land[pl.ds(LAND[k], half), :] + kept
            if k < 4:
                self.land[pl.ds(LAND[k], half), :] = total
            else:
                self.buf[self.rows(self.offs[5], half), :] = total

    def advance(self, k):
        if k > 0:
            self.finish(k - 1)
        if k < 10:
            self.copy(k).start()


def add_table(pos_s, idx_ref, table_s, first):
    row = lax.broadcasted_iota(jnp.int32, (table_s.shape[1], idx_ref.shape[1]), 0)
    acc = table_s[...]
    for j in range(TABLE_STEP):
        m = first + j
        hot = jnp.where(row == idx_ref[pl.ds(m, 1), :], 1.0, 0.0).astype(BF)
        val = pos_s[m]
        hi = val.astype(BF)
        rest = val - hi.astype(F32)
        mid = rest.astype(BF)
        low = (rest - mid.astype(F32)).astype(BF)
        acc = acc + dot_nt(jnp.concatenate([hi, mid, low], axis=0), hot)
    table_s[...] = acc


def reduce_kernel(*refs, n, n_small, bands):
    refs = list(refs)
    take = lambda count: [refs.pop(0) for _ in range(count)]
    pairs, smalls, (perm_ref, nm_ref, wr_ref, gpos_ref, idx_ref, res_in) = take(2 * n), take(n_small), take(6)
    outs, (small_out, res_out, gtok_out), held = take(n), take(3), take(2 * n)
    buf, land, small_land, pos_s, table_s, idx_s, send, recv, small_send, small_recv, sem_in, sem_out, res_send, res_recv, res_here, gnm_s, stage, sem_stage = refs
    seq = idx_ref.shape[0]
    n_heads = pos_s.shape[1]
    total = buf.shape[0]
    loads = [pltpu.make_async_copy(a, b, sem_in.at[i]) for i, (a, b) in enumerate(zip(pairs, held))]
    for load in loads:
        load.start()
    groups, base = [], 0
    for i, out in enumerate(outs):
        count = out.shape[0] * out.shape[1] // (512 * WIDTH)
        groups.append((base, count, held[2 * i], held[2 * i + 1], out, loads[2 * i:2 * i + 2]))
        base += count

    def block(out, j, side):
        wide = out.shape[1] // WIDTH
        row0, col0 = j // wide * 512 + side * 256, j % wide * WIDTH
        return out.at[pl.ds(pl.multiple_of(row0, 256), 256), pl.ds(pl.multiple_of(col0, WIDTH), WIDTH)]

    def part(ref, j):
        return ref[...] if ref.shape[1] == WIDTH else ref[:, pl.ds(pl.multiple_of(j * WIDTH, WIDTH), WIDTH)]

    peers = place()[1]
    dp, sp = lax.axis_index('dp'), lax.axis_index('sp')
    ring = res_in.shape[0]
    barrier = pltpu.get_barrier_semaphore()
    for peer in [peers[k] for k in ORDERS[0]] + [(dp, 3 - sp)]:
        pl.semaphore_signal(barrier, inc=1, device_id=peer, device_id_type=pl.DeviceIdType.MESH)
    pl.semaphore_wait(barrier, 6)
    moves = [pltpu.make_async_copy(res_in.at[sp], res_out.at[sp], res_here.at[0])]
    for d in range(1, ring):
        to = lax.rem(sp + d, ring)
        moves.append(pltpu.make_async_remote_copy(src_ref=res_in.at[to], dst_ref=res_out.at[sp], send_sem=res_send.at[d], recv_sem=res_recv.at[d],
                                                  device_id=(dp, to), device_id_type=pl.DeviceIdType.MESH))
    for move in moves:
        move.start()
    table_s[...] = jnp.zeros(table_s.shape, F32)
    room = small_out.shape[0] - table_s.shape[0] * table_s.shape[1] // (3 * 128)
    small_out[0:room, :] = jnp.zeros((room, 128), F32)
    gnm_s[...] = jnp.zeros(gnm_s.shape, F32)
    rows_of = small_rows([x.shape for x in smalls] + [gnm_s.shape])
    for ref, r, c, at in rows_of:
        if ref < n_small:
            small_out[at:at + 1, :] = smalls[ref][r:r + 1, c:c + 128]
    table_ticks = seq // TABLE_STEP
    small_at = TABLE_FROM + table_ticks + 1
    slots = total // 2

    def tick(t, carry):
        for k in range(10, -1, -1):
            u = t - STARTS[k]

            @pl.when((u >= 0) & (u < slots))
            def _():
                for side in range(2):
                    s = 2 * u + side
                    Stream(ORDERS[side], ORDERS[2 + side], lax.rem(u, Z_FIRST) == Z_FIRST - 1, buf.at[s], land.at[s], send.at[s], recv.at[s]).advance(k)
                if k == 10:
                    for first, count, left, right, out, loads in groups:
                        @pl.when((u >= first) & (u < first + count))
                        def _():
                            for side in range(2):
                                s = 2 * u + side
                                pltpu.make_async_copy(buf.at[s], block(out, u - first, side), sem_out.at[s]).start()

            @pl.when(t == small_at + k)
            def _():
                Stream(ORDERS[0], ORDERS[0], None, small_out, small_land, small_send, small_recv).advance(k)

        for first, count, left, right, out, loads in groups:
            @pl.when(t == (first if left is not held[-2] else 1))
            def _():
                for load in loads:
                    load.wait()

            @pl.when((t >= first) & (t < first + count))
            def _():
                value = dot_tn(part(left, t - first), part(right, t - first))
                buf[2 * t] = value[:256]
                buf[2 * t + 1] = value[256:]

        @pl.when(t == 0)
        def _():
            idx_s[...] = idx_ref[...].T
            for g in range(gpos_ref.shape[0]):
                for h in range(HEAD_GROUP):
                    pos_s[:, g * HEAD_GROUP + h, :] = gpos_ref[g, :, h * seq:(h + 1) * seq]

        @pl.when((lax.rem(t, 2) == 1) & (t < 2 * bands))
        def _():
            b = t // 2
            size = held[-1].shape[0] // bands
            store = pltpu.make_async_copy(stage, gtok_out.at[b], sem_stage.at[0])

            @pl.when(b > 0)
            def _():
                store.wait()
            merge_backward(pl.ds(pl.multiple_of(b * size, size), size), held[-2], held[-1], perm_ref, nm_ref, wr_ref, gnm_s, stage)
            store.start()

        @pl.when((t >= TABLE_FROM) & (t < TABLE_FROM + table_ticks))
        def _():
            add_table(pos_s, idx_s, table_s, (t - TABLE_FROM) * TABLE_STEP)

        @pl.when(t == TABLE_FROM + table_ticks)
        def _():
            for ref, r, c, at in rows_of:
                if ref == n_small:
                    small_out[at:at + 1, :] = gnm_s[r:r + 1, c:c + 128]
            summed = table_s[0:n_heads] + table_s[n_heads:2 * n_heads] + table_s[2 * n_heads:3 * n_heads]
            for p in range(table_s.shape[1] // 128):
                small_out[room + p * n_heads:room + (p + 1) * n_heads, :] = summed[:, p * 128:(p + 1) * 128]
        return carry
    lax.fori_loop(0, max(slots + STARTS[10] + 1, small_at + 11), tick, 0)

    def drain(s, carry):
        pltpu.make_async_copy(buf.at[s], block(outs[0], 0, 0), sem_out.at[s]).wait()
        return carry
    lax.fori_loop(0, total, drain, 0)
    for move in moves:
        move.wait()
    pltpu.make_async_copy(stage, gtok_out.at[bands - 1], sem_stage.at[0]).wait()


def small_rows(shapes):
    rows = []
    for ref, shape in enumerate(shapes):
        for r in range(shape[0]):
            for c in range(0, shape[1], 128):
                rows.append((ref, r, c, len(rows)))
    return rows


def reduce_all(pairs, smalls, extras, result, tokens, n_heads, table_len):
    shapes = [(a.shape[1], b.shape[1]) for a, b in pairs]
    total = sum(a * b // (256 * WIDTH) for a, b in shapes)
    n = len(pairs)
    flat = [x for pair in pairs for x in pair]
    seq = extras[-1].shape[0]
    table_pad = -(-table_len // 128) * 128
    vmem, hbm = pl.BlockSpec(memory_space=pltpu.VMEM), pl.BlockSpec(memory_space=pl.ANY)
    outs = [sds(shape, F32) for shape in shapes] + [sds((256, 128), F32), sds(result.shape, result.dtype), sds(tokens.shape, BF)]
    dma = pltpu.SemaphoreType.DMA
    ring = result.shape[0]
    return pl.pallas_call(
        functools.partial(reduce_kernel, n=n, n_small=len(smalls), bands=tokens.shape[0]),
        in_specs=[hbm] * (2 * n) + [vmem] * (len(smalls) + 5) + [hbm], out_specs=[hbm] * n + [vmem, hbm, hbm], out_shape=outs,
        scratch_shapes=[pltpu.VMEM(x.shape, x.dtype) for x in flat] + [
            pltpu.VMEM((total, 256, WIDTH), F32), pltpu.VMEM((total, 248, WIDTH), F32), pltpu.VMEM((248, 128), F32), pltpu.VMEM((seq, n_heads, seq), F32),
            pltpu.VMEM((3 * n_heads, table_pad), F32), pltpu.VMEM((seq, seq), jnp.int32), dma((total, 10)), dma((total, 10)), dma((10,)), dma((10,)),
            dma((2 * n,)), dma((total,)), dma((ring,)), dma((ring,)), dma((1,)),
            pltpu.VMEM(extras[1].shape, F32), pltpu.VMEM(tokens.shape[1:], BF), dma((1,))],
        name="reduce", compiler_params=pltpu.CompilerParams(collective_id=0, has_side_effects=True, vmem_limit_bytes=63 * 1024 * 1024))(
            *flat, *smalls, *extras, result)


def finish_kernel(*refs, n, cuts):
    refs = list(refs)
    take = lambda count: [refs.pop(0) for _ in range(count)]
    ins, (small,), outs, smalls, (table,), bufs, (sem_in, sem_out) = take(n), take(1), take(n), take(len(refs) - n - 3), take(1), take(n), refs
    stores = []
    loads = []
    for i, (a, b, c) in enumerate(zip(ins, bufs, outs)):
        step = a.shape[0] // cuts
        for p in range(cuts):
            at = pl.ds(p * step, step)
            loads.append(pltpu.make_async_copy(a.at[at], b.at[at], sem_in.at[i, p]))
            stores.append(pltpu.make_async_copy(b.at[at], c.at[at], sem_out.at[i, p]))
    for load in loads:
        load.start()
    for ref, r, c, at in small_rows([x.shape for x in smalls]):
        smalls[ref][r:r + 1, c:c + 128] = small[at:at + 1, :]
    n_heads, table_len = table.shape
    pieces = -(-table_len // 128)
    first = small.shape[0] - pieces * n_heads
    full = jnp.concatenate([small[first + p * n_heads:first + (p + 1) * n_heads, :] for p in range(pieces)], axis=1)
    table[...] = full[:, :table_len]
    for load, store in zip(loads, stores):
        load.wait()
        store.start()
    for store in stores:
        store.wait()


def finish(large, small, small_shapes, n_heads, table_len):
    n, cuts = len(large), 4
    vmem, hbm = pl.BlockSpec(memory_space=pltpu.VMEM), pl.BlockSpec(memory_space=pl.ANY)
    outs = [sds(x.shape, x.dtype) for x in large] + [sds(shape, F32) for shape in small_shapes] + [sds((n_heads, table_len), F32)]
    got = pl.pallas_call(
        functools.partial(finish_kernel, n=n, cuts=cuts), in_specs=[hbm] * n + [vmem], out_specs=[hbm] * n + [vmem] * (len(outs) - n), out_shape=outs,
        scratch_shapes=[pltpu.VMEM(x.shape, x.dtype) for x in large] + [pltpu.SemaphoreType.DMA((n, cuts)), pltpu.SemaphoreType.DMA((n, cuts))],
        name="finish", compiler_params=pltpu.CompilerParams(vmem_limit_bytes=VMEM_LIMIT))(*large, small)
    return got[:n], got[n:-1], got[-1].T


def solution(mesh):
    def device_fn(tokens, grad_out, rel_index, *weights):
        cot = lax.all_to_all(grad_out, 'sp', 1, 0, tiled=True)
        result, pairs, smalls, extras = local_step(tokens, cot, rel_index, weights)
        table_len, n_heads = weights[5].shape
        *grads, small, result, g_tok = reduce_all(pairs, smalls, extras, result, tokens, n_heads, table_len)
        small_shapes = [x.shape for x in smalls] + [weights[0].shape]
        large, smalls, g_table = finish(grads + [result, g_tok], small, small_shapes, n_heads, table_len)
        g_w2, g_w1, g_wq, g_wp, g_wr, result, g_tok = large
        g_na, g_nb, g_bq, g_bp, g_b1, g_b2, g_nm = smalls
        return (result.reshape(grad_out.shape), g_tok, g_nm, g_wr, g_na, g_wq, g_bq.reshape(-1), g_table, g_wp, g_bp.reshape(-1), g_nb,
                g_w1, g_b1.reshape(-1), g_w2, g_b2.reshape(-1))

    rep_specs = (P(),) * 13
    return jax.shard_map(device_fn, mesh=mesh, in_specs=(P('dp', 'sp'), P(('dp', 'sp')), P()) + rep_specs, out_specs=(P(('dp', 'sp')), P('dp', 'sp')) + rep_specs, check_vma=False)
```
